512 devices in a mesh: gx: 32 (over z, x_lo), gy: 16 (over y, x_hi, core).
Axes of the slice: x: 4 (x_hi: 2, x_lo: 2; x = x_hi * 2 + x_lo), y: 4, z: 16, core: 2. Of those that a mesh axis runs over, the one named last changes fastest.
Arguments:
- field: float32 [256, 128, 192], P('gx', 'gy'), may hold values from -6 to 6
- target: float32 [256, 128, 192], P('gx', 'gy'), may hold values from -6 to 6
- embed_weight: float32 [192, 256], replicated, may hold values from -0.4375 to 0.4375
- norm_gain: float32 [256], replicated, may hold values from 0.5 to 1.5
- attend_weight: float32 [256, 768], replicated, may hold values from -0.375 to 0.375
- output_weight: float32 [256, 256], replicated, may hold values from -0.375 to 0.375
- second_gain: float32 [256], replicated, may hold values from 0.5 to 1.5
- expand_weight: float32 [256, 512], replicated, may hold values from -0.375 to 0.375
- reduce_weight: float32 [512, 256], replicated, may hold values from -0.25 to 0.25
- decode_weight: float32 [256, 192], replicated, may hold values from -0.375 to 0.375
Outputs:
- loss: float32 [], replicated
- field_gradient: float32 [256, 128, 192], P('gx', 'gy')
- embed_gradient: float32 [192, 256], replicated
- norm_gradient: float32 [256], replicated
- attend_gradient: float32 [256, 768], replicated
- output_gradient: float32 [256, 256], replicated
- second_gradient: float32 [256], replicated
- expand_gradient: float32 [256, 512], replicated
- reduce_gradient: float32 [512, 256], replicated
- decode_gradient: float32 [256, 192], replicated
The draws below stay inside these ranges and needn't reach their ends.
All inputs are finite; a program needn't handle non-finite values.
Results may differ from the reference program's by a relative error of at most 0.0001.
Values sent between devices are 32-bit elements; how exact they have to be, the bound alone decides.
No kernel may reach another device: no remote copies, remote signals or barrier semaphores. Data moves between devices by JAX's collectives and lax.ppermute only.
A program may use at most 128 MiB of HBM per device.

```python
import jax
import jax.numpy as jnp
from jax import lax

NZ = 64
PATCH = 4
D = 256
HEADS = 8
FF = 512
STEPS = 2
NX = 256
NY = 128
CELLS = 6291456


def steps_of(key, dims, pieces, low, largest):
    level = 1.0
    for position, parts in pieces:
        heights = jax.random.uniform(jax.random.fold_in(jax.random.fold_in(key, 6), position), (parts,), jnp.float32, low / len(pieces), largest / len(pieces))
        level = level * jnp.repeat(jnp.exp(heights), dims[position] // parts).reshape((-1,) + (1,) * (len(dims) - 1 - position))
    return level


def bell_draw(rng, extent, scale, most, split=(), held_as=jnp.bfloat16):
    level = steps_of(rng, extent, split, -0.22, 0.18) if split else 1.0
    drawn = jax.random.normal(rng, extent, jnp.float32) * scale * level
    return jnp.minimum(jnp.maximum(drawn, -most), most).astype(held_as)


def setup_inputs(seed: int = 0) -> dict:
    arg_keys = jax.random.split(jax.random.key(seed), 11)
    field = bell_draw(arg_keys[0], (NX, NY, 3 * NZ), 1.0, 6.0, ((0, 32), (1, 16)), jnp.float32)
    target = bell_draw(arg_keys[1], (NX, NY, 3 * NZ), 1.0, 6.0, ((0, 32), (1, 16)), jnp.float32)
    embed_weight = bell_draw(arg_keys[2], (3 * PATCH * PATCH * PATCH, D), (3 * PATCH * PATCH * PATCH) ** -0.5, 0.4375, (), jnp.float32)
    norm_gain = jnp.clip(1.0 + 0.1 * jax.random.normal(arg_keys[3], (D,), jnp.float32), 0.5, 1.5)
    attend_weight = bell_draw(arg_keys[4], (D, 3 * D), D ** -0.5, 0.375, (), jnp.float32)
    output_weight = bell_draw(arg_keys[5], (D, D), D ** -0.5, 0.375, (), jnp.float32)
    second_gain = jnp.clip(1.0 + 0.1 * jax.random.normal(arg_keys[6], (D,), jnp.float32), 0.5, 1.5)
    expand_weight = bell_draw(arg_keys[7], (D, FF), D ** -0.5, 0.375, (), jnp.float32)
    reduce_weight = bell_draw(arg_keys[8], (FF, D), FF ** -0.5, 0.25, (), jnp.float32)
    decode_weight = bell_draw(arg_keys[9], (D, 3 * PATCH * PATCH * PATCH), D ** -0.5, 0.375, (), jnp.float32)
    return dict(field=field, target=target, embed_weight=embed_weight, norm_gain=norm_gain, attend_weight=attend_weight, output_weight=output_weight, second_gain=second_gain, expand_weight=expand_weight, reduce_weight=reduce_weight, decode_weight=decode_weight)


EXACT = lax.Precision.HIGHEST
EPSILON = 1e-06
TIME_STEP = 0.1
VISCOSITY = 0.5

def matmul(left, right):
    return jnp.dot(left, right, precision=EXACT)

def rms_scale(values, gain):
    power = lax.optimization_barrier(jnp.mean(values * values, axis=-1, keepdims=True))
    return values * lax.rsqrt(power + EPSILON) * gain

def closure(ext, params):
    embed_weight, norm_gain, attend_weight, output_weight, second_gain, expand_weight, reduce_weight, decode_weight = params
    wide, tall, depth = ext.shape
    levels = depth // 3
    across, along, upward = (wide // PATCH, tall // PATCH, levels // PATCH)
    patches = ext.reshape(across, PATCH, along, PATCH, 3, upward, PATCH).transpose(0, 2, 5, 4, 1, 3, 6)
    patches = patches.reshape(across, along, upward, 3 * PATCH * PATCH * PATCH)
    tokens = matmul(patches, embed_weight)
    width = tokens.shape[-1]
    head_size = width // HEADS
    mixed = matmul(rms_scale(tokens, norm_gain), attend_weight)
    inner_x, inner_y = (across - 2, along - 2)
    queries = mixed[1:-1, 1:-1, :, :width].reshape(inner_x, inner_y, upward, HEADS, head_size)
    keyset = mixed[:, :, :, width:2 * width]
    valset = mixed[:, :, :, 2 * width:]
    offsets = [(shift_x, shift_y) for shift_x in range(3) for shift_y in range(3)]
    keyblock = jnp.concatenate([keyset[sx:sx + inner_x, sy:sy + inner_y] for sx, sy in offsets], axis=2)
    valblock = jnp.concatenate([valset[sx:sx + inner_x, sy:sy + inner_y] for sx, sy in offsets], axis=2)
    keyblock = keyblock.reshape(inner_x, inner_y, 9 * upward, HEADS, head_size)
    valblock = valblock.reshape(inner_x, inner_y, 9 * upward, HEADS, head_size)
    factor = head_size ** (-0.5)
    scores = jnp.einsum('xyzhe,xywhe->xyhzw', queries, keyblock, precision=EXACT) * factor
    weights = jnp.exp(scores)
    weights = weights / lax.optimization_barrier(jnp.sum(weights, axis=-1, keepdims=True))
    attended = jnp.einsum('xyhzw,xywhe->xyzhe', weights, valblock, precision=EXACT)
    attended = attended.reshape(inner_x, inner_y, upward, width)
    middle = tokens[1:-1, 1:-1] + matmul(attended, output_weight)
    hidden = jax.nn.silu(matmul(rms_scale(middle, second_gain), expand_weight))
    middle = middle + matmul(hidden, reduce_weight)
    result = matmul(middle, decode_weight).reshape(inner_x, inner_y, upward, 3, PATCH, PATCH, PATCH)
    return result.transpose(0, 4, 1, 5, 3, 2, 6).reshape(inner_x * PATCH, inner_y * PATCH, depth)

def advance(ext, params):
    wide, tall, depth = ext.shape
    levels = depth // 3
    inner = ext[PATCH:wide - PATCH, PATCH:tall - PATCH]
    east = ext[PATCH + 1:wide - PATCH + 1, PATCH:tall - PATCH]
    west = ext[PATCH - 1:wide - PATCH - 1, PATCH:tall - PATCH]
    north = ext[PATCH:wide - PATCH, PATCH + 1:tall - PATCH + 1]
    south = ext[PATCH:wide - PATCH, PATCH - 1:tall - PATCH - 1]
    level = jnp.arange(depth, dtype=jnp.int32) % levels
    blank = jnp.zeros(inner.shape[:2] + (1,), jnp.float32)
    upper = jnp.where(level == levels - 1, 0.0, jnp.concatenate([inner[:, :, 1:], blank], axis=2))
    lower = jnp.where(level == 0, 0.0, jnp.concatenate([blank, inner[:, :, :-1]], axis=2))
    laplace = east + west + north + south + upper + lower - 6.0 * inner
    speed_x = jnp.concatenate([inner[:, :, 0:levels]] * 3, axis=2)
    speed_y = jnp.concatenate([inner[:, :, levels:2 * levels]] * 3, axis=2)
    speed_z = jnp.concatenate([inner[:, :, 2 * levels:]] * 3, axis=2)
    carried = 0.5 * (speed_x * (east - west) + speed_y * (north - south) + speed_z * (upper - lower))
    return inner + TIME_STEP * (VISCOSITY * laplace - carried + closure(ext, params))

def reference(field, target, embed_weight, norm_gain, attend_weight, output_weight, second_gain, expand_weight, reduce_weight, decode_weight):
    params = (embed_weight, norm_gain, attend_weight, output_weight, second_gain, expand_weight, reduce_weight, decode_weight)

    def misfit_of(start, weights):
        current = start
        for step in range(STEPS):
            padded = jnp.pad(current, ((PATCH, PATCH), (PATCH, PATCH), (0, 0)), mode='wrap')
            current = jax.checkpoint(advance)(padded, weights)
        residue = current - target
        return jnp.sum(residue * residue)
    misfit, pullback = jax.vjp(misfit_of, field, params)
    energy = jnp.sum(target * target)
    field_back, param_back = pullback(jnp.float32(1.0))
    scale = jnp.float32(CELLS) / energy
    loss = misfit / energy
    return (loss, scale * field_back, scale * param_back[0], scale * param_back[1], scale * param_back[2], scale * param_back[3], scale * param_back[4], scale * param_back[5], scale * param_back[6], scale * param_back[7])
```

```python
import jax
import jax.numpy as jnp
from jax import lax
from jax.experimental import pallas as pl
from jax.experimental.pallas import tpu as pltpu
from jax.sharding import Mesh, PartitionSpec as P

F32 = jnp.float32
BF16 = jnp.bfloat16
EPSILON = 1e-06
FACTOR = 32 ** (-0.5)
INTERPRET = False

EMBED, ATTEND, OUTPUT, EXPAND, REDUCE, DECODE, SMALL, ROWS = 0, 192, 960, 1216, 1728, 2240, 2432, 2560
VMEM_LIMIT = 60 * 1024 * 1024


def split(x):
    high = x.astype(BF16)
    return high, (x - high.astype(F32)).astype(BF16)


def dot(a, b, ca=1, cb=0):
    dims = (((ca,), (cb,)), ((), ()))

    def one(left, right):
        return lax.dot_general(left, right, dims, preferred_element_type=F32)

    return one(a[0], b[0]) + (one(a[0], b[1]) + one(a[1], b[0]))


def lanes(shape):
    return lax.broadcasted_iota(jnp.int32, shape, 1)


def over_components(x):
    x = x + pltpu.roll(x, 128, 1)
    return x + pltpu.roll(x, 64, 1)


def to_tokens(block_ref, rows_ref, turned_ref, out_ref):
    for px in range(2):
        for py in range(2):
            for dx in range(4):
                row = (px * 2 + py) * 16 + dx * 4
                rows_ref[row : row + 4, :] = block_ref[px * 4 + dx, py * 4 : py * 4 + 4, :]
    turned_ref[:, 0:64] = rows_ref[...].T
    turned_ref[:, 64:128] = jnp.zeros((192, 64), F32)
    lane = lanes((16, 128))
    halves = [[jnp.zeros((16, 128), F32) for _ in range(2)] for _ in range(4)]
    for c in range(3):
        for dz in range(4):
            piece = turned_ref[pl.ds(c * 64 + dz, 16, stride=4), :]
            place = c * 64 + dz * 16
            half, low = place // 128, place % 128
            chosen = (lane >= low) & (lane < low + 16)
            for column in range(4):
                shift = (low - column * 16) % 128
                moved = pltpu.roll(piece, shift, 1) if shift else piece
                halves[column][half] = jnp.where(chosen, moved, halves[column][half])
    for column in range(4):
        for half in range(2):
            out_ref[column * 16 : column * 16 + 16, half * 128 : half * 128 + 128] = halves[column][half]


def prepare_kernel(field_ref, target_ref, tokens_ref, goal_ref, rows_ref, turned_ref):
    to_tokens(field_ref, rows_ref, turned_ref, tokens_ref)
    to_tokens(target_ref, rows_ref, turned_ref, goal_ref)


def restore_kernel(a_ref, b_ref, c_ref, out_ref, turned_ref, rows_ref):
    total = a_ref[...] + (b_ref[...] + c_ref[...])
    lane = lanes((16, 128))
    for c in range(3):
        for dz in range(4):
            place = c * 64 + dz * 16
            half, low = place // 128, place % 128
            piece = jnp.zeros((16, 128), F32)
            for column in range(4):
                source = total[column * 16 : column * 16 + 16, half * 128 : half * 128 + 128]
                shift = (column * 16 - low) % 128
                moved = pltpu.roll(source, shift, 1) if shift else source
                chosen = (lane >= column * 16) & (lane < column * 16 + 16)
                piece = jnp.where(chosen, moved, piece)
            turned_ref[pl.ds(c * 64 + dz, 16, stride=4), :] = piece
    rows_ref[...] = turned_ref[...].T
    for px in range(2):
        for py in range(2):
            for dx in range(4):
                row = (px * 2 + py) * 16 + dx * 4
                out_ref[px * 4 + dx, py * 4 : py * 4 + 4, :] = rows_ref[row : row + 4, :]


def inner_rows(ref, m, n, dx=0, dy=0):
    width = ref.shape[1]
    parts = [ref[((X + 1 + dx) * m + 1 + dy) * 16 : ((X + 1 + dx) * m + 1 + dy + n) * 16, :] for X in range(n)]
    return jnp.concatenate(parts, axis=0)


def add_inner(ref, m, n, value, dx=0, dy=0):
    for X in range(n):
        start = ((X + 1 + dx) * m + 1 + dy) * 16
        ref[start : start + n * 16, :] += value[X * n * 16 : (X + 1) * n * 16]


def neighbours(ext_ref, m, n):
    count = n * n * 16
    lane = lanes((count, 256))
    row = lax.broadcasted_iota(jnp.int32, (count, 256), 0)
    dx, dy, dz, pz = (lane // 4) % 4, lane % 4, (lane // 16) % 4, row % 16
    here = inner_rows(ext_ref, m, n)
    roll = pltpu.roll
    east = jnp.where(dx < 3, roll(here, 252, 1), roll(inner_rows(ext_ref, m, n, 1, 0), 12, 1))
    west = jnp.where(dx > 0, roll(here, 4, 1), roll(inner_rows(ext_ref, m, n, -1, 0), 244, 1))
    north = jnp.where(dy < 3, roll(here, 255, 1), roll(inner_rows(ext_ref, m, n, 0, 1), 3, 1))
    south = jnp.where(dy > 0, roll(here, 1, 1), roll(inner_rows(ext_ref, m, n, 0, -1), 253, 1))
    above = jnp.where(pz == 15, 0.0, roll(here, count - 1, 0))
    below = jnp.where(pz == 0, 0.0, roll(here, 1, 0))
    upper = jnp.where(dz < 3, roll(here, 240, 1), roll(above, 48, 1))
    lower = jnp.where(dz > 0, roll(here, 16, 1), roll(below, 208, 1))
    speeds = [over_components(jnp.where(lane // 64 == k, here, 0.0)) for k in range(3)]
    return here, (east, west, north, south, upper, lower), speeds


def stencil(ext_ref, m, n):
    here, (east, west, north, south, upper, lower), speeds = neighbours(ext_ref, m, n)
    laplace = (east + west) + (north + south) + (upper + lower) - 6.0 * here
    carried = speeds[0] * (east - west) + speeds[1] * (north - south) + speeds[2] * (upper - lower)
    return here + 0.05 * (laplace - carried)


def stencil_back(ext_ref, back_ref, g, m, n):
    count = n * n * 16
    lane = lanes((count, 256))
    row = lax.broadcasted_iota(jnp.int32, (count, 256), 0)
    dx, dy, dz, pz = (lane // 4) % 4, lane % 4, (lane // 16) % 4, row % 16
    comp = lane // 64
    roll = pltpu.roll
    here, (east, west, north, south, upper, lower), speeds = neighbours(ext_ref, m, n)
    scaled = 0.05 * g
    own = 0.7 * g
    for k, (ahead, behind) in enumerate(((east, west), (north, south), (upper, lower))):
        own = own - jnp.where(comp == k, over_components(scaled * (ahead - behind)), 0.0)
    plus, minus = scaled * (1.0 - speeds[0]), scaled * (1.0 + speeds[0])
    own = own + jnp.where(dx > 0, roll(plus, 4, 1), 0.0) + jnp.where(dx < 3, roll(minus, 252, 1), 0.0)
    add_inner(back_ref, m, n, jnp.where(dx == 0, roll(plus, 244, 1), 0.0), 1, 0)
    add_inner(back_ref, m, n, jnp.where(dx == 3, roll(minus, 12, 1), 0.0), -1, 0)
    plus, minus = scaled * (1.0 - speeds[1]), scaled * (1.0 + speeds[1])
    own = own + jnp.where(dy > 0, roll(plus, 1, 1), 0.0) + jnp.where(dy < 3, roll(minus, 255, 1), 0.0)
    add_inner(back_ref, m, n, jnp.where(dy == 0, roll(plus, 253, 1), 0.0), 0, 1)
    add_inner(back_ref, m, n, jnp.where(dy == 3, roll(minus, 3, 1), 0.0), 0, -1)
    plus, minus = scaled * (1.0 - speeds[2]), scaled * (1.0 + speeds[2])
    own = own + jnp.where(dz > 0, roll(plus, 16, 1), 0.0) + jnp.where(dz < 3, roll(minus, 240, 1), 0.0)
    across = jnp.where(dz == 0, roll(plus, 208, 1), 0.0)
    own = own + jnp.where(pz == 0, 0.0, roll(across, 1, 0))
    across = jnp.where(dz == 3, roll(minus, 48, 1), 0.0)
    own = own + jnp.where(pz == 15, 0.0, roll(across, count - 1, 0))
    add_inner(back_ref, m, n, own)


def rms(x):
    return lax.rsqrt(jnp.mean(x * x, axis=1, keepdims=True) + EPSILON)


def rms_back(values, scale, gain, cotangent):
    weighted = cotangent * gain
    shared = jnp.mean(weighted * values, axis=1, keepdims=True)
    return scale * (weighted - values * (scale * scale * shared))


def pair(ref, start, size):
    return ref[0, pl.ds(start, size), :], ref[1, pl.ds(start, size), :]


def put(ref, start, value):
    high, low = split(value)
    ref[0, pl.ds(start, value.shape[0]), :] = high
    ref[1, pl.ds(start, value.shape[0]), :] = low


def both(ref):
    return ref[0], ref[1]


def head_mask():
    row = lax.broadcasted_iota(jnp.int32, (128, 256), 0)
    return row // 16 == lanes((128, 256)) // 32


def by_head(x, mask):
    wide = jnp.where(mask, jnp.concatenate([x] * 8, axis=0), 0.0)
    return split(wide)


def from_heads(x, mask):
    kept = jnp.where(mask, x, 0.0)
    total = kept[0:16]
    for head in range(1, 8):
        total = total + kept[head * 16 : head * 16 + 16]
    return total


def key_rows(X, Y, m):
    return [pl.multiple_of(((X + dx) * m + Y) * 16, 16) for dx in range(3)]


def gather(ref, starts, low, high):
    def one(which):
        return jnp.concatenate([ref[which, pl.ds(s, 48), low:high] for s in starts], axis=0)

    return one(0), one(1)


def forward(w, g1, g2, ext_ref, r, m, n, chunk):
    (tok, nrm, kv, q, wts, att, mid, h, late) = r

    def embed(i, _):
        start = pl.multiple_of(i * chunk, chunk)
        tokens = dot(split(ext_ref[pl.ds(start, chunk), :]), both(w["embed"]))
        tok[pl.ds(start, chunk), :] = tokens
        normed = tokens * rms(tokens) * g1
        put(nrm, start, normed)
        put(kv, start, dot(pair(nrm, start, chunk), (w["attend"][0, :, 256:], w["attend"][1, :, 256:])))
        return 0

    lax.fori_loop(0, m * m * 16 // chunk, embed, 0)
    normed_in = inner_rows(nrm.at[0], m, n), inner_rows(nrm.at[1], m, n)
    q[...] = dot(normed_in, (w["attend"][0, :, :256], w["attend"][1, :, :256]))
    mask = head_mask()

    def attend(i, _):
        X, Y = i // n, i % n
        starts = key_rows(X, Y, m)
        here = pl.multiple_of(i * 16, 16)
        wide = by_head(q[pl.ds(here, 16), :], mask)
        scores = dot(gather(kv, starts, 0, 256), wide, 1, 1)
        weights = jnp.exp(scores * FACTOR)
        weights = weights / jnp.sum(weights, axis=0, keepdims=True)
        wts[i] = weights
        att[pl.ds(here, 16), :] = from_heads(dot(split(weights), gather(kv, starts, 256, 512), 0, 0), mask)
        return 0

    lax.fori_loop(0, n * n, attend, 0)
    middle = inner_rows(tok, m, n) + dot(split(att[...]), both(w["output"]))
    mid[...] = middle
    hidden = dot(split(middle * rms(middle) * g2), both(w["expand"]))
    h[...] = hidden
    active = hidden / (1.0 + jnp.exp(-hidden))
    final = middle + dot(split(active), both(w["reduce"]))
    late[...] = final
    return dot(split(final), both(w["decode"]), 1, 1)


def add_rows(ref, start, value, first):
    size = value.shape[0]
    if first:
        ref[start : start + size, :] = value
    else:
        ref[start : start + size, :] += value


def reorder(strip, source, inverse=False):
    places = [(c * 64 + dz * 16, c * 64 + dz) for c in range(3) for dz in range(4)]
    halves = []
    for k in range(2):
        part = source[:, 128 * k : 128 * k + 128]
        if inverse:
            for place, row in places:
                strip[k, pl.ds(row, 16, stride=4), :] = part[place : place + 16]
            halves.append(strip[k])
        else:
            strip[k] = part
            halves.append(jnp.concatenate([strip[k, pl.ds(row, 16, stride=4), :] for _, row in places], axis=0))
    return jnp.concatenate(halves, axis=1)


def backward(w, g1, g2, ext_ref, back_ref, grads, r, dkv, dq, g, m, n, chunk, first):
    (tok, nrm, kv, q, wts, att, mid, h, late) = r
    dclosure = split(0.1 * g)
    add_rows(grads, DECODE, dot(dclosure, split(late[...]), 0, 0)[:192], first)
    dmid = dot(dclosure, both(w["decode"]))
    back = split(dmid)
    hidden = h[...]
    gate = 1.0 / (1.0 + jnp.exp(-hidden))
    add_rows(grads, REDUCE, dot(split(hidden * gate), back, 0, 0), first)
    dhidden = split(dot(back, both(w["reduce"]), 1, 1) * (gate * (1.0 + hidden * (1.0 - gate))))
    middle = mid[...]
    scale = rms(middle)
    second = split(middle * scale * g2)
    add_rows(grads, EXPAND, dot(second, (dhidden[0][:, :256], dhidden[1][:, :256]), 0, 0), first)
    add_rows(grads, EXPAND + 256, dot(second, (dhidden[0][:, 256:], dhidden[1][:, 256:]), 0, 0), first)
    dsecond = dot(dhidden, both(w["expand"]), 1, 1)
    add_rows(grads, SMALL + 1, jnp.sum(dsecond * middle * scale, axis=0, keepdims=True), first)
    dmid = dmid + rms_back(middle, scale, g2, dsecond)
    back = split(dmid)
    add_rows(grads, OUTPUT, dot(split(att[...]), back, 0, 0), first)
    att[...] = dot(back, both(w["output"]), 1, 1)
    dkv[...] = jnp.zeros(dkv.shape, F32)
    mask = head_mask()

    def attend(i, _):
        X, Y = i // n, i % n
        starts = key_rows(X, Y, m)
        here = pl.multiple_of(i * 16, 16)
        wide = by_head(q[pl.ds(here, 16), :], mask)
        dwide = by_head(att[pl.ds(here, 16), :], mask)
        weights = wts[i]
        dweights = dot(gather(kv, starts, 256, 512), dwide, 1, 1)
        common = jnp.sum(weights * dweights, axis=0, keepdims=True)
        dscores = split(weights * (dweights - common) * FACTOR)
        dq[pl.ds(here, 16), :] = from_heads(dot(dscores, gather(kv, starts, 0, 256), 0, 0), mask)
        dkeys = dot(dscores, wide)
        dvals = dot(split(weights), dwide)
        for k, s in enumerate(starts):
            dkv[pl.ds(s, 48), 0:256] += dkeys[k * 48 : k * 48 + 48]
            dkv[pl.ds(s, 48), 256:512] += dvals[k * 48 : k * 48 + 48]
        return 0

    lax.fori_loop(0, n * n, attend, 0)
    normed_in = inner_rows(nrm.at[0], m, n), inner_rows(nrm.at[1], m, n)
    dquery = split(dq[...])
    add_rows(grads, ATTEND, dot(normed_in, dquery, 0, 0), first)
    back_ref[...] = jnp.zeros(back_ref.shape, F32)
    add_inner(back_ref, m, n, dot(dquery, (w["attend"][0, :, :256], w["attend"][1, :, :256]), 1, 1))
    total = dkv[...]
    halves = [split(total[:, 0:256]), split(total[:, 256:512])]
    normed = both(nrm)
    for k in range(2):
        add_rows(grads, ATTEND + 256 + 256 * k, dot(normed, halves[k], 0, 0), first)
    dnormed = back_ref[...]
    for k in range(2):
        low, high = 256 + 256 * k, 512 + 256 * k
        dnormed = dnormed + dot(halves[k], (w["attend"][0, :, low:high], w["attend"][1, :, low:high]), 1, 1)
    tokens = tok[...]
    scale = rms(tokens)
    add_rows(grads, SMALL, jnp.sum(dnormed * tokens * scale, axis=0, keepdims=True), first)
    back_ref[...] = rms_back(tokens, scale, g1, dnormed)
    add_inner(back_ref, m, n, dmid)
    dtokens = split(back_ref[...])
    add_rows(grads, EMBED, dot(split(ext_ref[...]), dtokens, 0, 0)[:192], first)
    back_ref[...] = dot(dtokens, both(w["embed"]), 1, 1)
    stencil_back(ext_ref, back_ref, g, m, n)


def main_kernel(*refs):
    (low, own, high, goal, embed, gain1, attend, output, gain2, expand, reduce, decode) = refs[:12]
    (grads, out_low, out_own, out_high) = refs[12:16]
    scratch = list(refs[16:])
    w = {}
    for name in ("embed", "attend", "output", "expand", "reduce", "decode"):
        w[name] = scratch.pop(0)
    strip = scratch.pop(0)
    ext0, back0, ext1, back1, dkv0, dkv1, dq0, dq1 = scratch[:8]
    r0, r1 = scratch[8:17], scratch[17:26]
    put(w["embed"], 0, reorder(strip, embed[...]))
    put(w["decode"], 0, reorder(strip, decode[...].T))
    put(w["embed"], 192, jnp.zeros((64, 256), F32))
    put(w["decode"], 192, jnp.zeros((64, 256), F32))
    put(w["attend"], 0, attend[...])
    put(w["output"], 0, output[...])
    put(w["expand"], 0, expand[...])
    put(w["reduce"], 0, reduce[...])
    g1, g2 = gain1[...], gain2[...]
    places = [
        (by, bx, (px * 2 + py) * 16, ((2 * bx + px) * 6 + 2 * by + py) * 16)
        for by in range(3) for bx in range(3) for px in range(2) for py in range(2)
    ]
    for by, bx, source, place in places:
        ext0[place : place + 16, :] = (low, own, high)[by][bx, source : source + 16, :]
    ext1[...] = stencil(ext0, 6, 4) + 0.1 * forward(w, g1, g2, ext0, r0, 6, 4, 192)
    final = stencil(ext1, 4, 2) + 0.1 * forward(w, g1, g2, ext1, r1, 4, 2, 128)
    residue = final - goal[...]
    grads[SMALL:ROWS, :] = jnp.zeros((ROWS - SMALL, 256), F32)
    sums = [jnp.sum(jnp.sum(v * v, axis=0, keepdims=True), axis=1, keepdims=True) for v in (residue, goal[...])]
    lane = lanes((1, 256))
    grads[SMALL + 2 : SMALL + 3, :] = jnp.where(lane == 0, sums[0], jnp.where(lane == 1, sums[1], 0.0))
    backward(w, g1, g2, ext1, back1, grads, r1, dkv1, dq1, 2.0 * residue, 4, 2, 128, True)
    backward(w, g1, g2, ext0, back0, grads, r0, dkv0, dq0, back1[...], 6, 4, 192, False)
    for by, bx, source, place in places:
        (out_low, out_own, out_high)[by][bx, source : source + 16, :] = back0[place : place + 16, :]


def finish_kernel(core, mine, other, loss, embed, norm, attend, output, second, expand, reduce, decode, strip, red):
    first = core[0] == 0
    red[0 : ROWS // 2, :] = jnp.where(first, mine[...], other[...])
    red[ROWS // 2 :, :] = jnp.where(first, other[...], mine[...])
    misfit = red[SMALL + 2 : SMALL + 3, 0:1]
    energy = red[SMALL + 2 : SMALL + 3, 1:2]
    scale = 6291456.0 / energy
    loss[...] = jnp.where(lanes((1, 128)) == 0, misfit / energy, scale)
    embed[...] = scale * reorder(strip, red[EMBED:ATTEND, :], True)
    for k in range(3):
        attend[:, 256 * k : 256 * k + 256] = scale * red[ATTEND + 256 * k : ATTEND + 256 * k + 256, :]
    output[...] = scale * red[OUTPUT:EXPAND, :]
    for k in range(2):
        expand[:, 256 * k : 256 * k + 256] = scale * red[EXPAND + 256 * k : EXPAND + 256 * k + 256, :]
    reduce[...] = scale * red[REDUCE:DECODE, :]
    decode[...] = (scale * reorder(strip, red[DECODE:SMALL, :], True)).T
    norm[...] = scale * red[SMALL : SMALL + 1, :]
    second[...] = scale * red[SMALL + 1 : SMALL + 2, :]


def arr(*shape, dtype=F32):
    return jax.ShapeDtypeStruct(shape, dtype)


def call(kernel, outs, scratch, name, **more):
    return pl.pallas_call(
        kernel,
        out_shape=outs,
        scratch_shapes=scratch,
        compiler_params=pltpu.CompilerParams(vmem_limit_bytes=VMEM_LIMIT),
        name=name,
        interpret=INTERPRET,
        **more,
    )


def prepare(field, target):
    scratch = [pltpu.VMEM((64, 192), F32), pltpu.VMEM((192, 128), F32)]
    return call(prepare_kernel, (arr(64, 256), arr(64, 256)), scratch, "prepare")(field, target)


def work(low, own, high, goal, weights):
    def V(*shape, dtype=F32):
        return pltpu.VMEM(shape, dtype)

    def kept(te, ti, n):
        return [
            V(te, 256), V(2, te, 256, dtype=BF16), V(2, te, 512, dtype=BF16), V(ti, 256), V(n * n, 144, 128),
            V(ti, 256), V(ti, 256), V(ti, 512), V(ti, 256),
        ]

    scratch = [
        V(2, 256, 256, dtype=BF16), V(2, 256, 768, dtype=BF16), V(2, 256, 256, dtype=BF16),
        V(2, 256, 512, dtype=BF16), V(2, 512, 256, dtype=BF16), V(2, 256, 256, dtype=BF16),
        V(2, 192, 128),
        V(576, 256), V(576, 256), V(256, 256), V(256, 256), V(576, 512), V(256, 512), V(256, 256), V(64, 256),
        *kept(576, 256, 4), *kept(256, 64, 2),
    ]
    outs = (arr(ROWS, 256), arr(3, 64, 256), arr(3, 64, 256), arr(3, 64, 256))
    embed, gain1, attend, output, gain2, expand, reduce, decode = weights
    args = (embed, gain1.reshape(1, 256), attend, output, gain2.reshape(1, 256), expand, reduce, decode)
    return call(main_kernel, outs, scratch, "work")(low, own, high, goal, *args)


def restore(a, b, c):
    scratch = [pltpu.VMEM((192, 128), F32), pltpu.VMEM((128, 192), F32)]
    return call(restore_kernel, arr(8, 8, 192), scratch, "restore")(a, b, c)


def finish(mine, other, core):
    outs = (
        arr(1, 128), arr(192, 256), arr(1, 256), arr(256, 768), arr(256, 256), arr(1, 256), arr(256, 512),
        arr(512, 256), arr(256, 192),
    )
    scratch = [pltpu.VMEM((2, 192, 128), F32), pltpu.VMEM((ROWS, 256), F32)]
    specs = [pl.BlockSpec(memory_space=pltpu.SMEM)] + [pl.BlockSpec(memory_space=pltpu.VMEM)] * 2
    return call(finish_kernel, outs, scratch, "finish", in_specs=specs)(core, mine, other)


AXES = ("z", "xl", "y", "xh", "co")
GX, GY = ("z", "xl"), ("y", "xh", "co")


def shift(x, axes, step):
    count = lax.axis_size(axes)
    return lax.ppermute(x, axes, [(i, (i + step) % count) for i in range(count)])


PLANE = ("xl", "y", "xh")


def swap(x, axes):
    return lax.all_to_all(x, axes, 0, 0, tiled=True)


def reduce_all(grads):
    core = lax.axis_index("co")
    halves = grads.reshape(2, ROWS // 2, 256)
    kept = lax.dynamic_index_in_dim(halves, core, 0, keepdims=False)
    sent = lax.dynamic_index_in_dim(halves, 1 - core, 0, keepdims=False)
    total = kept + lax.ppermute(sent, "co", [(0, 1), (1, 0)])
    total = jnp.sum(swap(total.reshape(16, ROWS // 32, 256), PLANE), axis=0)
    total = jnp.sum(swap(total.reshape(16, ROWS // 512, 256), "z"), axis=0)
    total = swap(jnp.broadcast_to(total, (16,) + total.shape), "z").reshape(ROWS // 32, 256)
    total = swap(jnp.broadcast_to(total, (16,) + total.shape), PLANE).reshape(ROWS // 2, 256)
    return total, lax.ppermute(total, "co", [(0, 1), (1, 0)])


def shards(field, target, *weights):
    tokens, goal = prepare(field, target)
    own = jnp.stack([shift(tokens, GX, 1), tokens, shift(tokens, GX, -1)])
    low, high = shift(own, GY, 1), shift(own, GY, -1)
    grads, back_low, back_own, back_high = work(low, own, high, goal, weights)
    mine, other = reduce_all(grads)
    wide = back_own + (shift(back_low, GY, -1) + shift(back_high, GY, 1))
    spread = restore(wide[1], shift(wide[0], GX, -1), shift(wide[2], GX, 1))
    loss, embed, norm, attend, output, second, expand, reduce, decode = finish(mine, other, lax.axis_index("co").reshape(1))
    field_back = loss[0, 1] * spread
    return loss[0, 0], field_back, embed, norm[0], attend, output, second[0], expand, reduce, decode


def solution(mesh):
    fine = Mesh(mesh.devices.reshape(16, 2, 4, 2, 2), AXES)
    block = P(GX, GY, None)
    in_specs = (block, block) + (P(),) * 8
    out_specs = (P(), block) + (P(),) * 8
    return jax.shard_map(shards, mesh=fine, in_specs=in_specs, out_specs=out_specs, check_vma=False)
```

```python
import jax
import jax.numpy as jnp
from jax import lax
from jax.experimental import pallas as pl
from jax.experimental.pallas import tpu as pltpu
from jax.sharding import Mesh, PartitionSpec as P

F32 = jnp.float32
BF16 = jnp.bfloat16
EPSILON = 1e-06
FACTOR = 32 ** (-0.5)
INTERPRET = False

EMBED, ATTEND, OUTPUT, EXPAND, REDUCE, DECODE, SMALL, ROWS = 0, 192, 960, 1216, 1728, 2240, 2432, 2560
VMEM_LIMIT = 60 * 1024 * 1024


def split(x):
    high = x.astype(BF16)
    return high, (x - high.astype(F32)).astype(BF16)


def dot(a, b, ca=1, cb=0):
    dims = (((ca,), (cb,)), ((), ()))

    def one(left, right):
        return lax.dot_general(left, right, dims, preferred_element_type=F32)

    return one(a[0], b[0]) + (one(a[0], b[1]) + one(a[1], b[0]))


def lanes(shape):
    return lax.broadcasted_iota(jnp.int32, shape, 1)


def over_components(x):
    x = x + pltpu.roll(x, 128, 1)
    return x + pltpu.roll(x, 64, 1)


def to_tokens(block_ref, rows_ref, turned_ref, out_ref):
    for px in range(2):
        for py in range(2):
            for dx in range(4):
                row = (px * 2 + py) * 16 + dx * 4
                rows_ref[row : row + 4, :] = block_ref[px * 4 + dx, py * 4 : py * 4 + 4, :]
    turned_ref[:, 0:64] = rows_ref[...].T
    turned_ref[:, 64:128] = jnp.zeros((192, 64), F32)
    lane = lanes((16, 128))
    halves = [[jnp.zeros((16, 128), F32) for _ in range(2)] for _ in range(4)]
    for c in range(3):
        for dz in range(4):
            piece = turned_ref[pl.ds(c * 64 + dz, 16, stride=4), :]
            place = c * 64 + dz * 16
            half, low = place // 128, place % 128
            chosen = (lane >= low) & (lane < low + 16)
            for column in range(4):
                shift = (low - column * 16) % 128
                moved = pltpu.roll(piece, shift, 1) if shift else piece
                halves[column][half] = jnp.where(chosen, moved, halves[column][half])
    for column in range(4):
        for half in range(2):
            out_ref[column * 16 : column * 16 + 16, half * 128 : half * 128 + 128] = halves[column][half]


def prepare_kernel(field_ref, target_ref, tokens_ref, goal_ref, rows_ref, turned_ref):
    to_tokens(field_ref, rows_ref, turned_ref, tokens_ref)
    to_tokens(target_ref, rows_ref, turned_ref, goal_ref)


def from_tokens(total, out_ref, turned_ref, rows_ref):
    lane = lanes((16, 128))
    for c in range(3):
        for dz in range(4):
            place = c * 64 + dz * 16
            half, low = place // 128, place % 128
            piece = jnp.zeros((16, 128), F32)
            for column in range(4):
                source = total[column * 16 : column * 16 + 16, half * 128 : half * 128 + 128]
                shift = (column * 16 - low) % 128
                moved = pltpu.roll(source, shift, 1) if shift else source
                chosen = (lane >= column * 16) & (lane < column * 16 + 16)
                piece = jnp.where(chosen, moved, piece)
            turned_ref[pl.ds(c * 64 + dz, 16, stride=4), :] = piece
    rows_ref[...] = turned_ref[...].T
    for px in range(2):
        for py in range(2):
            for dx in range(4):
                row = (px * 2 + py) * 16 + dx * 4
                out_ref[px * 4 + dx, py * 4 : py * 4 + 4, :] = rows_ref[row : row + 4, :]


def inner_rows(ref, m, n, dx=0, dy=0):
    parts = [ref[((X + 1 + dx) * m + 1 + dy) * 16 : ((X + 1 + dx) * m + 1 + dy + n) * 16, :] for X in range(n)]
    return jnp.concatenate(parts, axis=0)


def add_inner(ref, m, n, value, dx=0, dy=0):
    for X in range(n):
        start = ((X + 1 + dx) * m + 1 + dy) * 16
        ref[start : start + n * 16, :] += value[X * n * 16 : (X + 1) * n * 16]


def neighbours(ext_ref, m, n):
    count = n * n * 16
    lane = lanes((count, 256))
    row = lax.broadcasted_iota(jnp.int32, (count, 256), 0)
    dx, dy, dz, pz = (lane // 4) % 4, lane % 4, (lane // 16) % 4, row % 16
    here = inner_rows(ext_ref, m, n)
    roll = pltpu.roll
    east = jnp.where(dx < 3, roll(here, 252, 1), roll(inner_rows(ext_ref, m, n, 1, 0), 12, 1))
    west = jnp.where(dx > 0, roll(here, 4, 1), roll(inner_rows(ext_ref, m, n, -1, 0), 244, 1))
    north = jnp.where(dy < 3, roll(here, 255, 1), roll(inner_rows(ext_ref, m, n, 0, 1), 3, 1))
    south = jnp.where(dy > 0, roll(here, 1, 1), roll(inner_rows(ext_ref, m, n, 0, -1), 253, 1))
    above = jnp.where(pz == 15, 0.0, roll(here, count - 1, 0))
    below = jnp.where(pz == 0, 0.0, roll(here, 1, 0))
    upper = jnp.where(dz < 3, roll(here, 240, 1), roll(above, 48, 1))
    lower = jnp.where(dz > 0, roll(here, 16, 1), roll(below, 208, 1))
    speeds = [over_components(jnp.where(lane // 64 == k, here, 0.0)) for k in range(3)]
    return here, (east, west, north, south, upper, lower), speeds


def stencil(ext_ref, m, n):
    here, (east, west, north, south, upper, lower), speeds = neighbours(ext_ref, m, n)
    laplace = (east + west) + (north + south) + (upper + lower) - 6.0 * here
    carried = speeds[0] * (east - west) + speeds[1] * (north - south) + speeds[2] * (upper - lower)
    return here + 0.05 * (laplace - carried)


def stencil_back(ext_ref, back_ref, g, m, n):
    count = n * n * 16
    lane = lanes((count, 256))
    row = lax.broadcasted_iota(jnp.int32, (count, 256), 0)
    dx, dy, dz, pz = (lane // 4) % 4, lane % 4, (lane // 16) % 4, row % 16
    comp = lane // 64
    roll = pltpu.roll
    here, (east, west, north, south, upper, lower), speeds = neighbours(ext_ref, m, n)
    scaled = 0.05 * g
    own = 0.7 * g
    for k, (ahead, behind) in enumerate(((east, west), (north, south), (upper, lower))):
        own = own - jnp.where(comp == k, over_components(scaled * (ahead - behind)), 0.0)
    plus, minus = scaled * (1.0 - speeds[0]), scaled * (1.0 + speeds[0])
    own = own + jnp.where(dx > 0, roll(plus, 4, 1), 0.0) + jnp.where(dx < 3, roll(minus, 252, 1), 0.0)
    add_inner(back_ref, m, n, jnp.where(dx == 0, roll(plus, 244, 1), 0.0), 1, 0)
    add_inner(back_ref, m, n, jnp.where(dx == 3, roll(minus, 12, 1), 0.0), -1, 0)
    plus, minus = scaled * (1.0 - speeds[1]), scaled * (1.0 + speeds[1])
    own = own + jnp.where(dy > 0, roll(plus, 1, 1), 0.0) + jnp.where(dy < 3, roll(minus, 255, 1), 0.0)
    add_inner(back_ref, m, n, jnp.where(dy == 0, roll(plus, 253, 1), 0.0), 0, 1)
    add_inner(back_ref, m, n, jnp.where(dy == 3, roll(minus, 3, 1), 0.0), 0, -1)
    plus, minus = scaled * (1.0 - speeds[2]), scaled * (1.0 + speeds[2])
    own = own + jnp.where(dz > 0, roll(plus, 16, 1), 0.0) + jnp.where(dz < 3, roll(minus, 240, 1), 0.0)
    across = jnp.where(dz == 0, roll(plus, 208, 1), 0.0)
    own = own + jnp.where(pz == 0, 0.0, roll(across, 1, 0))
    across = jnp.where(dz == 3, roll(minus, 48, 1), 0.0)
    own = own + jnp.where(pz == 15, 0.0, roll(across, count - 1, 0))
    add_inner(back_ref, m, n, own)


def rms(x):
    return lax.rsqrt(jnp.mean(x * x, axis=1, keepdims=True) + EPSILON)


def rms_back(values, scale, gain, cotangent):
    weighted = cotangent * gain
    shared = jnp.mean(weighted * values, axis=1, keepdims=True)
    return scale * (weighted - values * (scale * scale * shared))


def pair(ref, start, size):
    return ref[0, pl.ds(start, size), :], ref[1, pl.ds(start, size), :]


def put(ref, start, value):
    high, low = split(value)
    ref[0, pl.ds(start, value.shape[0]), :] = high
    ref[1, pl.ds(start, value.shape[0]), :] = low


def both(ref):
    return ref[0], ref[1]


def head_mask():
    row = lax.broadcasted_iota(jnp.int32, (128, 256), 0)
    return row // 16 == lanes((128, 256)) // 32


def pair_mask():
    key = lax.broadcasted_iota(jnp.int32, (192, 256), 0) // 16 % 4
    query = lanes((192, 256)) // 128
    return (key >= query) & (key < query + 3)


def by_head(x, mask):
    wide = [jnp.where(mask, jnp.concatenate([x[k * 16 : k * 16 + 16]] * 8, axis=0), 0.0) for k in range(2)]
    return split(jnp.concatenate(wide, axis=0))


def from_heads(x, mask):
    columns = []
    for k in range(2):
        kept = jnp.where(mask, x[128 * k : 128 * k + 128], 0.0)
        total = [kept[head * 16 : head * 16 + 16] for head in range(8)]
        while len(total) > 1:
            total = [total[i] + total[i + 1] for i in range(0, len(total), 2)]
        columns.append(total[0])
    return jnp.concatenate(columns, axis=0)


def key_rows(X, Y, m):
    return [((X + dx) * m + Y) * 16 for dx in range(3)]


def gather(ref, starts, low, high):
    def one(which):
        return jnp.concatenate([ref[which, s : s + 64, low:high] for s in starts], axis=0)

    return one(0), one(1)


def pairs_of(n):
    return [(X, Y) for X in range(n) for Y in range(0, n, 2)]


def forward(w, g1, g2, ext_ref, r, m, n, chunk):
    (tok, nrm, kv, q, wts, att, mid, h, late) = r

    def embed(i, _):
        start = pl.multiple_of(i * chunk, chunk)
        tokens = dot(split(ext_ref[pl.ds(start, chunk), :]), both(w["embed"]))
        tok[pl.ds(start, chunk), :] = tokens
        normed = tokens * rms(tokens) * g1
        put(nrm, start, normed)
        put(kv, start, dot(pair(nrm, start, chunk), (w["attend"][0, :, 256:], w["attend"][1, :, 256:])))
        return 0

    lax.fori_loop(0, m * m * 16 // chunk, embed, 0)
    normed_in = inner_rows(nrm.at[0], m, n), inner_rows(nrm.at[1], m, n)
    q[...] = dot(normed_in, (w["attend"][0, :, :256], w["attend"][1, :, :256]))
    mask = head_mask()

    allowed = pair_mask()

    def attend(pairs):
        results = []
        for X, Y in pairs:
            starts = key_rows(X, Y, m)
            wide = by_head(q[(X * n + Y) * 16 : (X * n + Y) * 16 + 32, :], mask)
            weights = jnp.where(allowed, jnp.exp(dot(gather(kv, starts, 0, 256), wide, 1, 1) * FACTOR), 0.0)
            weights = weights / jnp.sum(weights, axis=0, keepdims=True)
            results.append((weights, from_heads(dot(split(weights), gather(kv, starts, 256, 512), 0, 0), mask)))
        for (X, Y), (weights, attended) in zip(pairs, results):
            wts[X * (n // 2) + Y // 2] = weights
            att[(X * n + Y) * 16 : (X * n + Y) * 16 + 32, :] = attended

    attend(pairs_of(n))
    middle = inner_rows(tok, m, n) + dot(split(att[...]), both(w["output"]))
    mid[...] = middle
    hidden = dot(split(middle * rms(middle) * g2), both(w["expand"]))
    h[...] = hidden
    active = hidden / (1.0 + jnp.exp(-hidden))
    final = middle + dot(split(active), both(w["reduce"]))
    late[...] = final
    return dot(split(final), both(w["decode"]), 1, 1)


def add_rows(ref, start, value, first):
    size = value.shape[0]
    if first:
        ref[start : start + size, :] = value
    else:
        ref[start : start + size, :] += value


def reorder(strip, source, inverse=False):
    places = [(c * 64 + dz * 16, c * 64 + dz) for c in range(3) for dz in range(4)]
    halves = []
    for k in range(2):
        part = source[:, 128 * k : 128 * k + 128]
        if inverse:
            for place, row in places:
                strip[k, pl.ds(row, 16, stride=4), :] = part[place : place + 16]
            halves.append(strip[k])
        else:
            strip[k] = part
            halves.append(jnp.concatenate([strip[k, pl.ds(row, 16, stride=4), :] for _, row in places], axis=0))
    return jnp.concatenate(halves, axis=1)


def backward(w, g1, g2, ext_ref, back_ref, grads, r, dkv, dq, g, m, n, first):
    (tok, nrm, kv, q, wts, att, mid, h, late) = r
    dclosure = split(0.1 * g)
    add_rows(grads, DECODE, dot(dclosure, split(late[...]), 0, 0)[:192], first)
    dmid = dot(dclosure, both(w["decode"]))
    back = split(dmid)
    hidden = h[...]
    gate = 1.0 / (1.0 + jnp.exp(-hidden))
    add_rows(grads, REDUCE, dot(split(hidden * gate), back, 0, 0), first)
    dhidden = split(dot(back, both(w["reduce"]), 1, 1) * (gate * (1.0 + hidden * (1.0 - gate))))
    middle = mid[...]
    scale = rms(middle)
    second = split(middle * scale * g2)
    add_rows(grads, EXPAND, dot(second, (dhidden[0][:, :256], dhidden[1][:, :256]), 0, 0), first)
    add_rows(grads, EXPAND + 256, dot(second, (dhidden[0][:, 256:], dhidden[1][:, 256:]), 0, 0), first)
    dsecond = dot(dhidden, both(w["expand"]), 1, 1)
    add_rows(grads, SMALL + 1, jnp.sum(dsecond * middle * scale, axis=0, keepdims=True), first)
    dmid = dmid + rms_back(middle, scale, g2, dsecond)
    back = split(dmid)
    add_rows(grads, OUTPUT, dot(split(att[...]), back, 0, 0), first)
    att[...] = dot(back, both(w["output"]), 1, 1)
    dkv[...] = jnp.zeros(dkv.shape, F32)
    mask = head_mask()

    def attend(pairs):
        results = []
        for X, Y in pairs:
            starts = key_rows(X, Y, m)
            here = slice((X * n + Y) * 16, (X * n + Y) * 16 + 32)
            wide, dwide = by_head(q[here, :], mask), by_head(att[here, :], mask)
            weights = wts[X * (n // 2) + Y // 2]
            dweights = dot(gather(kv, starts, 256, 512), dwide, 1, 1)
            common = jnp.sum(weights * dweights, axis=0, keepdims=True)
            dscores = split(weights * (dweights - common) * FACTOR)
            dqueries = from_heads(dot(dscores, gather(kv, starts, 0, 256), 0, 0), mask)
            results.append((dqueries, dot(dscores, wide), dot(split(weights), dwide)))
        for (X, Y), (dqueries, dkeys, dvals) in zip(pairs, results):
            dq[(X * n + Y) * 16 : (X * n + Y) * 16 + 32, :] = dqueries
            for k, s in enumerate(key_rows(X, Y, m)):
                dkv[s : s + 64, 0:256] += dkeys[k * 64 : k * 64 + 64]
                dkv[s : s + 64, 256:512] += dvals[k * 64 : k * 64 + 64]

    attend(pairs_of(n))
    normed_in = inner_rows(nrm.at[0], m, n), inner_rows(nrm.at[1], m, n)
    dquery = split(dq[...])
    add_rows(grads, ATTEND, dot(normed_in, dquery, 0, 0), first)
    back_ref[...] = jnp.zeros(back_ref.shape, F32)
    add_inner(back_ref, m, n, dot(dquery, (w["attend"][0, :, :256], w["attend"][1, :, :256]), 1, 1))
    total = dkv[...]
    halves = [split(total[:, 0:256]), split(total[:, 256:512])]
    normed = both(nrm)
    for k in range(2):
        add_rows(grads, ATTEND + 256 + 256 * k, dot(normed, halves[k], 0, 0), first)
    dnormed = back_ref[...]
    for k in range(2):
        low, high = 256 + 256 * k, 512 + 256 * k
        dnormed = dnormed + dot(halves[k], (w["attend"][0, :, low:high], w["attend"][1, :, low:high]), 1, 1)
    tokens = tok[...]
    scale = rms(tokens)
    add_rows(grads, SMALL, jnp.sum(dnormed * tokens * scale, axis=0, keepdims=True), first)
    back_ref[...] = rms_back(tokens, scale, g1, dnormed)
    add_inner(back_ref, m, n, dmid)
    dtokens = split(back_ref[...])
    add_rows(grads, EMBED, dot(split(ext_ref[...]), dtokens, 0, 0)[:192], first)
    back_ref[...] = dot(dtokens, both(w["embed"]), 1, 1)
    stencil_back(ext_ref, back_ref, g, m, n)


def main_kernel(*refs):
    (core, low, own, high, goal, embed, gain1, attend, output, gain2, expand, reduce, decode) = refs[:13]
    (kept, sent, out_low, out_own, out_high) = refs[13:18]
    scratch = list(refs[18:])
    grads = scratch.pop(0)
    w = {}
    for name in ("embed", "attend", "output", "expand", "reduce", "decode"):
        w[name] = scratch.pop(0)
    strip = scratch.pop(0)
    ext0, back0, ext1, back1, dkv0, dkv1, dq0, dq1 = scratch[:8]
    r0, r1 = scratch[8:17], scratch[17:26]
    put(w["embed"], 0, reorder(strip, embed[...]))
    put(w["decode"], 0, reorder(strip, decode[...]))
    put(w["embed"], 192, jnp.zeros((64, 256), F32))
    put(w["decode"], 192, jnp.zeros((64, 256), F32))
    put(w["attend"], 0, attend[...])
    put(w["output"], 0, output[...])
    put(w["expand"], 0, expand[...])
    put(w["reduce"], 0, reduce[...])
    g1, g2 = gain1[...], gain2[...]
    spots = [
        (by, bx, (px * 2 + py) * 16, ((2 * bx + px) * 6 + 2 * by + py) * 16)
        for by in range(3) for bx in range(3) for px in range(2) for py in range(2)
    ]
    for by, bx, source, place in spots:
        ext0[place : place + 16, :] = (low, own, high)[by][bx, source : source + 16, :]
    ext1[...] = stencil(ext0, 6, 4) + 0.1 * forward(w, g1, g2, ext0, r0, 6, 4, 192)
    final = stencil(ext1, 4, 2) + 0.1 * forward(w, g1, g2, ext1, r1, 4, 2, 128)
    residue = final - goal[...]
    grads[SMALL:ROWS, :] = jnp.zeros((ROWS - SMALL, 256), F32)
    sums = [jnp.sum(jnp.sum(v * v, axis=0, keepdims=True), axis=1, keepdims=True) for v in (residue, goal[...])]
    lane = lanes((1, 256))
    grads[SMALL + 2 : SMALL + 3, :] = jnp.where(lane == 0, sums[0], jnp.where(lane == 1, sums[1], 0.0))
    backward(w, g1, g2, ext1, back1, grads, r1, dkv1, dq1, 2.0 * residue, 4, 2, True)
    backward(w, g1, g2, ext0, back0, grads, r0, dkv0, dq0, back1[...], 6, 4, False)
    for by, bx, source, place in spots:
        (out_low, out_own, out_high)[by][bx, source : source + 16, :] = back0[place : place + 16, :]
    half = ROWS // 2
    kept[...] = grads[pl.ds(pl.multiple_of(core[0] * half, half), half), :]
    sent[...] = grads[pl.ds(pl.multiple_of((1 - core[0]) * half, half), half), :]


def finish_kernel(
    core, mine, other, wide, before, after,
    loss, field, embed, norm, attend, output, second, expand, reduce, decode, strip, red, turned, rows,
):
    first = core[0] == 0
    red[0 : ROWS // 2, :] = jnp.where(first, mine[...], other[...])
    red[ROWS // 2 :, :] = jnp.where(first, other[...], mine[...])
    misfit = red[SMALL + 2 : SMALL + 3, 0:1]
    energy = red[SMALL + 2 : SMALL + 3, 1:2]
    scale = 6291456.0 / energy
    loss[...] = misfit / energy
    from_tokens(scale * (wide[1] + (before[...] + after[...])), field, turned, rows)
    embed[...] = scale * reorder(strip, red[EMBED:ATTEND, :], True)
    for k in range(3):
        attend[:, 256 * k : 256 * k + 256] = scale * red[ATTEND + 256 * k : ATTEND + 256 * k + 256, :]
    output[...] = scale * red[OUTPUT:EXPAND, :]
    for k in range(2):
        expand[:, 256 * k : 256 * k + 256] = scale * red[EXPAND + 256 * k : EXPAND + 256 * k + 256, :]
    reduce[...] = scale * red[REDUCE:DECODE, :]
    decode[...] = scale * reorder(strip, red[DECODE:SMALL, :], True)
    norm[...] = scale * red[SMALL : SMALL + 1, :]
    second[...] = scale * red[SMALL + 1 : SMALL + 2, :]


def places(scalars, arrays):
    return [pl.BlockSpec(memory_space=pltpu.SMEM)] * scalars + [pl.BlockSpec(memory_space=pltpu.VMEM)] * arrays


def arr(*shape, dtype=F32):
    return jax.ShapeDtypeStruct(shape, dtype)


def call(kernel, outs, scratch, **more):
    return pl.pallas_call(
        kernel,
        out_shape=outs,
        scratch_shapes=scratch,
        compiler_params=pltpu.CompilerParams(vmem_limit_bytes=VMEM_LIMIT),
        interpret=INTERPRET,
        **more,
    )


def prepare(field, target):
    scratch = [pltpu.VMEM((64, 192), F32), pltpu.VMEM((192, 128), F32)]
    return call(prepare_kernel, (arr(64, 256), arr(64, 256)), scratch)(field, target)


def work(core, low, own, high, goal, weights):
    def V(*shape, dtype=F32):
        return pltpu.VMEM(shape, dtype)

    def kept(te, ti, n):
        return [
            V(te, 256), V(2, te, 256, dtype=BF16), V(2, te, 512, dtype=BF16), V(ti, 256), V(n * n // 2, 192, 256),
            V(ti, 256), V(ti, 256), V(ti, 512), V(ti, 256),
        ]

    scratch = [
        V(ROWS, 256), V(2, 256, 256, dtype=BF16), V(2, 256, 768, dtype=BF16), V(2, 256, 256, dtype=BF16),
        V(2, 256, 512, dtype=BF16), V(2, 512, 256, dtype=BF16), V(2, 256, 256, dtype=BF16),
        V(2, 192, 128),
        V(576, 256), V(576, 256), V(256, 256), V(256, 256), V(576, 512), V(256, 512), V(256, 256), V(64, 256),
        *kept(576, 256, 4), *kept(256, 64, 2),
    ]
    half = arr(ROWS // 2, 256)
    outs = (half, half, arr(3, 64, 256), arr(3, 64, 256), arr(3, 64, 256))
    embed, gain1, attend, output, gain2, expand, reduce, decode = weights
    args = (embed, gain1.reshape(1, 256), attend, output, gain2.reshape(1, 256), expand, reduce, decode.T)
    return call(main_kernel, outs, scratch, in_specs=places(1, 12))(core, low, own, high, goal, *args)


def finish(core, mine, other, wide, before, after):
    outs = (
        arr(1, 1), arr(8, 8, 192), arr(192, 256), arr(1, 256), arr(256, 768), arr(256, 256), arr(1, 256),
        arr(256, 512), arr(512, 256), arr(192, 256),
    )
    scratch = [
        pltpu.VMEM((2, 192, 128), F32), pltpu.VMEM((ROWS, 256), F32),
        pltpu.VMEM((192, 128), F32), pltpu.VMEM((128, 192), F32),
    ]
    return call(finish_kernel, outs, scratch, in_specs=places(1, 5))(core, mine, other, wide, before, after)


AXES = ("z", "xl", "y", "xh", "co")
GX, GY = ("z", "xl"), ("y", "xh", "co")


def shift(x, axes, step):
    count = lax.axis_size(axes)
    return lax.ppermute(x, axes, [(i, (i + step) % count) for i in range(count)])


PLANE = ("xl", "y", "xh")


def swap(x, axes):
    return lax.all_to_all(x, axes, 0, 0, tiled=True)


def shards(field, target, *weights):
    core = lax.axis_index("co").reshape(1)
    half = ROWS // 2
    swapped = [(0, 1), (1, 0)]
    tokens, goal = prepare(field, target)
    own = jnp.stack([shift(tokens, GX, 1), tokens, shift(tokens, GX, -1)])
    low, high = shift(own, GY, 1), shift(own, GY, -1)
    kept, sent, back_low, back_own, back_high = work(core, low, own, high, goal, weights)
    total = kept + lax.ppermute(sent, "co", swapped)
    back_low, back_high = shift(back_low, GY, -1), shift(back_high, GY, 1)
    wide = back_own + (back_low + back_high)
    total = jnp.sum(swap(total.reshape(16, half // 16, 256), PLANE), axis=0)
    before, after = shift(wide[0], GX, -1), shift(wide[2], GX, 1)
    total = jnp.sum(swap(total.reshape(16, half // 256, 256), "z"), axis=0)
    total = swap(jnp.broadcast_to(total, (16,) + total.shape), "z").reshape(half // 16, 256)
    total = swap(jnp.broadcast_to(total, (16,) + total.shape), PLANE).reshape(half, 256)
    other = lax.ppermute(total, "co", swapped)
    results = finish(core, total, other, wide, before, after)
    loss, field_back, embed, norm, attend, output, second, expand, reduce, decode = results
    return loss[0, 0], field_back, embed, norm[0], attend, output, second[0], expand, reduce, decode.T


def solution(mesh):
    fine = Mesh(mesh.devices.reshape(16, 2, 4, 2, 2), AXES)
    block = P(GX, GY, None)
    in_specs = (block, block) + (P(),) * 8
    out_specs = (P(), block) + (P(),) * 8
    return jax.shard_map(shards, mesh=fine, in_specs=in_specs, out_specs=out_specs, check_vma=False)
```

```python
import jax
import jax.numpy as jnp
from jax import lax
from jax.experimental import pallas as pl
from jax.experimental.pallas import tpu as pltpu
from jax.sharding import Mesh, PartitionSpec as P

F32 = jnp.float32
BF16 = jnp.bfloat16
EPSILON = 1e-06
FACTOR = 32 ** (-0.5)
INTERPRET = False

EMBED, ATTEND, OUTPUT, EXPAND, REDUCE, DECODE, SMALL, ROWS = 0, 192, 960, 1216, 1728, 2240, 2432, 2560
MIB = 1024 * 1024


def split(x):
    high = x.astype(BF16)
    return high, (x - high.astype(F32)).astype(BF16)


def dot(a, b, ca=1, cb=0):
    dims = (((ca,), (cb,)), ((), ()))

    def one(left, right):
        return lax.dot_general(left, right, dims, preferred_element_type=F32)

    return one(a[0], b[0]) + (one(a[0], b[1]) + one(a[1], b[0]))


def lanes(shape):
    return lax.broadcasted_iota(jnp.int32, shape, 1)


def over_components(x):
    x = x + pltpu.roll(x, 128, 1)
    return x + pltpu.roll(x, 64, 1)


def to_tokens(block_ref, rows_ref, turned_ref, out_ref):
    for px in range(2):
        for py in range(2):
            for dx in range(4):
                row = (px * 2 + py) * 16 + dx * 4
                rows_ref[row : row + 4, :] = block_ref[px * 4 + dx, py * 4 : py * 4 + 4, :]
    turned_ref[:, 0:64] = rows_ref[...].T
    turned_ref[:, 64:128] = jnp.zeros((192, 64), F32)
    lane = lanes((16, 128))
    halves = [[jnp.zeros((16, 128), F32) for _ in range(2)] for _ in range(4)]
    for c in range(3):
        for dz in range(4):
            piece = turned_ref[pl.ds(c * 64 + dz, 16, stride=4), :]
            place = c * 64 + dz * 16
            half, low = place // 128, place % 128
            chosen = (lane >= low) & (lane < low + 16)
            for column in range(4):
                shift = (low - column * 16) % 128
                moved = pltpu.roll(piece, shift, 1) if shift else piece
                halves[column][half] = jnp.where(chosen, moved, halves[column][half])
    for column in range(4):
        for half in range(2):
            out_ref[column * 16 : column * 16 + 16, half * 128 : half * 128 + 128] = halves[column][half]


def prepare_kernel(field_ref, target_ref, tokens_ref, goal_ref, rows_ref, turned_ref):
    to_tokens(field_ref, rows_ref, turned_ref, tokens_ref)
    to_tokens(target_ref, rows_ref, turned_ref, goal_ref)


def from_tokens(total, out_ref, turned_ref, rows_ref):
    lane = lanes((16, 128))
    for c in range(3):
        for dz in range(4):
            place = c * 64 + dz * 16
            half, low = place // 128, place % 128
            piece = jnp.zeros((16, 128), F32)
            for column in range(4):
                source = total[column * 16 : column * 16 + 16, half * 128 : half * 128 + 128]
                shift = (column * 16 - low) % 128
                moved = pltpu.roll(source, shift, 1) if shift else source
                chosen = (lane >= column * 16) & (lane < column * 16 + 16)
                piece = jnp.where(chosen, moved, piece)
            turned_ref[pl.ds(c * 64 + dz, 16, stride=4), :] = piece
    rows_ref[...] = turned_ref[...].T
    for px in range(2):
        for py in range(2):
            for dx in range(4):
                row = (px * 2 + py) * 16 + dx * 4
                out_ref[px * 4 + dx, py * 4 : py * 4 + 4, :] = rows_ref[row : row + 4, :]


def inner_rows(ref, m, n, dx=0, dy=0):
    parts = [ref[((X + 1 + dx) * m + 1 + dy) * 16 : ((X + 1 + dx) * m + 1 + dy + n) * 16, :] for X in range(n)]
    return jnp.concatenate(parts, axis=0)


def add_inner(ref, m, n, value, dx=0, dy=0):
    for X in range(n):
        start = ((X + 1 + dx) * m + 1 + dy) * 16
        ref[start : start + n * 16, :] += value[X * n * 16 : (X + 1) * n * 16]


def neighbours(ext_ref, m, n):
    count = n * n * 16
    lane = lanes((count, 256))
    row = lax.broadcasted_iota(jnp.int32, (count, 256), 0)
    dx, dy, dz, pz = (lane // 4) % 4, lane % 4, (lane // 16) % 4, row % 16
    here = inner_rows(ext_ref, m, n)
    roll = pltpu.roll
    east = jnp.where(dx < 3, roll(here, 252, 1), roll(inner_rows(ext_ref, m, n, 1, 0), 12, 1))
    west = jnp.where(dx > 0, roll(here, 4, 1), roll(inner_rows(ext_ref, m, n, -1, 0), 244, 1))
    north = jnp.where(dy < 3, roll(here, 255, 1), roll(inner_rows(ext_ref, m, n, 0, 1), 3, 1))
    south = jnp.where(dy > 0, roll(here, 1, 1), roll(inner_rows(ext_ref, m, n, 0, -1), 253, 1))
    above = jnp.where(pz == 15, 0.0, roll(here, count - 1, 0))
    below = jnp.where(pz == 0, 0.0, roll(here, 1, 0))
    upper = jnp.where(dz < 3, roll(here, 240, 1), roll(above, 48, 1))
    lower = jnp.where(dz > 0, roll(here, 16, 1), roll(below, 208, 1))
    speeds = [over_components(jnp.where(lane // 64 == k, here, 0.0)) for k in range(3)]
    return here, (east, west, north, south, upper, lower), speeds


def stencil(ext_ref, m, n):
    here, (east, west, north, south, upper, lower), speeds = neighbours(ext_ref, m, n)
    laplace = (east + west) + (north + south) + (upper + lower) - 6.0 * here
    carried = speeds[0] * (east - west) + speeds[1] * (north - south) + speeds[2] * (upper - lower)
    return here + 0.05 * (laplace - carried)


def stencil_back(ext_ref, back_ref, g, m, n):
    count = n * n * 16
    lane = lanes((count, 256))
    row = lax.broadcasted_iota(jnp.int32, (count, 256), 0)
    dx, dy, dz, pz = (lane // 4) % 4, lane % 4, (lane // 16) % 4, row % 16
    comp = lane // 64
    roll = pltpu.roll
    here, (east, west, north, south, upper, lower), speeds = neighbours(ext_ref, m, n)
    scaled = 0.05 * g
    own = 0.7 * g
    for k, (ahead, behind) in enumerate(((east, west), (north, south), (upper, lower))):
        own = own - jnp.where(comp == k, over_components(scaled * (ahead - behind)), 0.0)
    plus, minus = scaled * (1.0 - speeds[0]), scaled * (1.0 + speeds[0])
    own = own + jnp.where(dx > 0, roll(plus, 4, 1), 0.0) + jnp.where(dx < 3, roll(minus, 252, 1), 0.0)
    add_inner(back_ref, m, n, jnp.where(dx == 0, roll(plus, 244, 1), 0.0), 1, 0)
    add_inner(back_ref, m, n, jnp.where(dx == 3, roll(minus, 12, 1), 0.0), -1, 0)
    plus, minus = scaled * (1.0 - speeds[1]), scaled * (1.0 + speeds[1])
    own = own + jnp.where(dy > 0, roll(plus, 1, 1), 0.0) + jnp.where(dy < 3, roll(minus, 255, 1), 0.0)
    add_inner(back_ref, m, n, jnp.where(dy == 0, roll(plus, 253, 1), 0.0), 0, 1)
    add_inner(back_ref, m, n, jnp.where(dy == 3, roll(minus, 3, 1), 0.0), 0, -1)
    plus, minus = scaled * (1.0 - speeds[2]), scaled * (1.0 + speeds[2])
    own = own + jnp.where(dz > 0, roll(plus, 16, 1), 0.0) + jnp.where(dz < 3, roll(minus, 240, 1), 0.0)
    across = jnp.where(dz == 0, roll(plus, 208, 1), 0.0)
    own = own + jnp.where(pz == 0, 0.0, roll(across, 1, 0))
    across = jnp.where(dz == 3, roll(minus, 48, 1), 0.0)
    own = own + jnp.where(pz == 15, 0.0, roll(across, count - 1, 0))
    add_inner(back_ref, m, n, own)


def rms(x):
    return lax.rsqrt(jnp.mean(x * x, axis=1, keepdims=True) + EPSILON)


def rms_back(values, scale, gain, cotangent):
    weighted = cotangent * gain
    shared = jnp.mean(weighted * values, axis=1, keepdims=True)
    return scale * (weighted - values * (scale * scale * shared))


def pair(ref, start, size):
    return ref[0, pl.ds(start, size), :], ref[1, pl.ds(start, size), :]


def put(ref, start, value):
    high, low = split(value)
    ref[0, pl.ds(start, value.shape[0]), :] = high
    ref[1, pl.ds(start, value.shape[0]), :] = low


def both(ref):
    return ref[0], ref[1]


def head_mask():
    row = lax.broadcasted_iota(jnp.int32, (128, 256), 0)
    return row // 16 == lanes((128, 256)) // 32


def pair_mask():
    key = lax.broadcasted_iota(jnp.int32, (192, 256), 0) // 16 % 4
    query = lanes((192, 256)) // 128
    return (key >= query) & (key < query + 3)


def by_head(x, mask):
    wide = [jnp.where(mask, jnp.concatenate([x[k * 16 : k * 16 + 16]] * 8, axis=0), 0.0) for k in range(2)]
    return split(jnp.concatenate(wide, axis=0))


def from_heads(x, mask):
    columns = []
    for k in range(2):
        kept = jnp.where(mask, x[128 * k : 128 * k + 128], 0.0)
        total = [kept[head * 16 : head * 16 + 16] for head in range(8)]
        while len(total) > 1:
            total = [total[i] + total[i + 1] for i in range(0, len(total), 2)]
        columns.append(total[0])
    return jnp.concatenate(columns, axis=0)


def key_rows(X, Y, m):
    return [((X + dx) * m + Y) * 16 for dx in range(3)]


def gather(ref, starts, low, high):
    def one(which):
        return jnp.concatenate([ref[which, s : s + 64, low:high] for s in starts], axis=0)

    return one(0), one(1)


def pairs_of(n):
    return [(X, Y) for X in range(n) for Y in range(0, n, 2)]


def forward(w, g1, g2, ext_ref, r, m, n, chunk):
    (tok, nrm, kv, q, wts, att, mid, h, late) = r

    def embed(i, _):
        start = pl.multiple_of(i * chunk, chunk)
        tokens = dot(split(ext_ref[pl.ds(start, chunk), :]), both(w["embed"]))
        tok[pl.ds(start, chunk), :] = tokens
        normed = tokens * rms(tokens) * g1
        put(nrm, start, normed)
        put(kv, start, dot(pair(nrm, start, chunk), (w["attend"][0, :, 256:], w["attend"][1, :, 256:])))
        return 0

    lax.fori_loop(0, m * m * 16 // chunk, embed, 0)
    normed_in = inner_rows(nrm.at[0], m, n), inner_rows(nrm.at[1], m, n)
    q[...] = dot(normed_in, (w["attend"][0, :, :256], w["attend"][1, :, :256]))
    mask = head_mask()

    allowed = pair_mask()

    def attend(pairs):
        results = []
        for X, Y in pairs:
            starts = key_rows(X, Y, m)
            wide = by_head(q[(X * n + Y) * 16 : (X * n + Y) * 16 + 32, :], mask)
            weights = jnp.where(allowed, jnp.exp(dot(gather(kv, starts, 0, 256), wide, 1, 1) * FACTOR), 0.0)
            weights = weights / jnp.sum(weights, axis=0, keepdims=True)
            results.append((weights, from_heads(dot(split(weights), gather(kv, starts, 256, 512), 0, 0), mask)))
        for (X, Y), (weights, attended) in zip(pairs, results):
            wts[X * (n // 2) + Y // 2] = weights
            att[(X * n + Y) * 16 : (X * n + Y) * 16 + 32, :] = attended

    attend(pairs_of(n))
    middle = inner_rows(tok, m, n) + dot(split(att[...]), both(w["output"]))
    mid[...] = middle
    hidden = dot(split(middle * rms(middle) * g2), both(w["expand"]))
    h[...] = hidden
    active = hidden / (1.0 + jnp.exp(-hidden))
    final = middle + dot(split(active), both(w["reduce"]))
    late[...] = final
    return dot(split(final), both(w["decode"]), 1, 1)


def add_rows(ref, start, value, first):
    size = value.shape[0]
    if first:
        ref[start : start + size, :] = value
    else:
        ref[start : start + size, :] += value


def reorder(strip, source, inverse=False):
    places = [(c * 64 + dz * 16, c * 64 + dz) for c in range(3) for dz in range(4)]
    halves = []
    for k in range(2):
        part = source[:, 128 * k : 128 * k + 128]
        if inverse:
            for place, row in places:
                strip[k, pl.ds(row, 16, stride=4), :] = part[place : place + 16]
            halves.append(strip[k])
        else:
            strip[k] = part
            halves.append(jnp.concatenate([strip[k, pl.ds(row, 16, stride=4), :] for _, row in places], axis=0))
    return jnp.concatenate(halves, axis=1)


def backward(w, g1, g2, ext_ref, back_ref, grads, r, dkv, dq, g, m, n, first):
    (tok, nrm, kv, q, wts, att, mid, h, late) = r
    dclosure = split(0.1 * g)
    add_rows(grads, DECODE, dot(dclosure, split(late[...]), 0, 0)[:192], first)
    dmid = dot(dclosure, both(w["decode"]))
    back = split(dmid)
    hidden = h[...]
    gate = 1.0 / (1.0 + jnp.exp(-hidden))
    add_rows(grads, REDUCE, dot(split(hidden * gate), back, 0, 0), first)
    dhidden = split(dot(back, both(w["reduce"]), 1, 1) * (gate * (1.0 + hidden * (1.0 - gate))))
    middle = mid[...]
    scale = rms(middle)
    second = split(middle * scale * g2)
    add_rows(grads, EXPAND, dot(second, (dhidden[0][:, :256], dhidden[1][:, :256]), 0, 0), first)
    add_rows(grads, EXPAND + 256, dot(second, (dhidden[0][:, 256:], dhidden[1][:, 256:]), 0, 0), first)
    dsecond = dot(dhidden, both(w["expand"]), 1, 1)
    add_rows(grads, SMALL + 1, jnp.sum(dsecond * middle * scale, axis=0, keepdims=True), first)
    dmid = dmid + rms_back(middle, scale, g2, dsecond)
    back = split(dmid)
    add_rows(grads, OUTPUT, dot(split(att[...]), back, 0, 0), first)
    att[...] = dot(back, both(w["output"]), 1, 1)
    dkv[...] = jnp.zeros(dkv.shape, F32)
    mask = head_mask()

    def attend(pairs):
        results = []
        for X, Y in pairs:
            starts = key_rows(X, Y, m)
            here = slice((X * n + Y) * 16, (X * n + Y) * 16 + 32)
            wide, dwide = by_head(q[here, :], mask), by_head(att[here, :], mask)
            weights = wts[X * (n // 2) + Y // 2]
            dweights = dot(gather(kv, starts, 256, 512), dwide, 1, 1)
            common = jnp.sum(weights * dweights, axis=0, keepdims=True)
            dscores = split(weights * (dweights - common) * FACTOR)
            dqueries = from_heads(dot(dscores, gather(kv, starts, 0, 256), 0, 0), mask)
            results.append((dqueries, dot(dscores, wide), dot(split(weights), dwide)))
        for (X, Y), (dqueries, dkeys, dvals) in zip(pairs, results):
            dq[(X * n + Y) * 16 : (X * n + Y) * 16 + 32, :] = dqueries
            for k, s in enumerate(key_rows(X, Y, m)):
                dkv[s : s + 64, 0:256] += dkeys[k * 64 : k * 64 + 64]
                dkv[s : s + 64, 256:512] += dvals[k * 64 : k * 64 + 64]

    attend(pairs_of(n))
    normed_in = inner_rows(nrm.at[0], m, n), inner_rows(nrm.at[1], m, n)
    dquery = split(dq[...])
    add_rows(grads, ATTEND, dot(normed_in, dquery, 0, 0), first)
    back_ref[...] = jnp.zeros(back_ref.shape, F32)
    add_inner(back_ref, m, n, dot(dquery, (w["attend"][0, :, :256], w["attend"][1, :, :256]), 1, 1))
    total = dkv[...]
    halves = [split(total[:, 0:256]), split(total[:, 256:512])]
    normed = both(nrm)
    for k in range(2):
        add_rows(grads, ATTEND + 256 + 256 * k, dot(normed, halves[k], 0, 0), first)
    dnormed = back_ref[...]
    for k in range(2):
        low, high = 256 + 256 * k, 512 + 256 * k
        dnormed = dnormed + dot(halves[k], (w["attend"][0, :, low:high], w["attend"][1, :, low:high]), 1, 1)
    tokens = tok[...]
    scale = rms(tokens)
    add_rows(grads, SMALL, jnp.sum(dnormed * tokens * scale, axis=0, keepdims=True), first)
    back_ref[...] = rms_back(tokens, scale, g1, dnormed)
    add_inner(back_ref, m, n, dmid)
    dtokens = split(back_ref[...])
    add_rows(grads, EMBED, dot(split(ext_ref[...]), dtokens, 0, 0)[:192], first)
    back_ref[...] = dot(dtokens, both(w["embed"]), 1, 1)
    stencil_back(ext_ref, back_ref, g, m, n)


NAMES = ("embed", "attend", "output", "expand", "reduce", "decode")
WIDTHS = {"embed": (256, 256), "attend": (256, 768), "output": (256, 256), "expand": (256, 512), "reduce": (512, 256), "decode": (256, 256)}


def weights_kernel(*refs):
    inputs, w, strip = dict(zip(NAMES, refs[:6])), dict(zip(NAMES, refs[6:12])), refs[12]
    for name in NAMES:
        if name in ("embed", "decode"):
            put(w[name], 0, reorder(strip, inputs[name][...]))
            put(w[name], 192, jnp.zeros((64, 256), F32))
        else:
            put(w[name], 0, inputs[name][...])


def main_kernel(*refs):
    (core, low, own, high, goal, gain1, gain2) = refs[:7]
    w = dict(zip(NAMES, refs[7:13]))
    (kept, sent, out_low, out_own, out_high) = refs[13:18]
    scratch = list(refs[18:])
    grads = scratch.pop(0)
    ext0, back0, ext1, back1, dkv0, dkv1, dq0, dq1 = scratch[:8]
    r0, r1 = scratch[8:17], scratch[17:26]
    g1, g2 = gain1[...], gain2[...]
    spots = [
        (by, bx, (px * 2 + py) * 16, ((2 * bx + px) * 6 + 2 * by + py) * 16)
        for by in range(3) for bx in range(3) for px in range(2) for py in range(2)
    ]
    for by, bx, source, place in spots:
        ext0[place : place + 16, :] = (low, own, high)[by][bx, source : source + 16, :]
    ext1[...] = stencil(ext0, 6, 4) + 0.1 * forward(w, g1, g2, ext0, r0, 6, 4, 192)
    final = stencil(ext1, 4, 2) + 0.1 * forward(w, g1, g2, ext1, r1, 4, 2, 128)
    residue = final - goal[...]
    grads[SMALL:ROWS, :] = jnp.zeros((ROWS - SMALL, 256), F32)
    sums = [jnp.sum(jnp.sum(v * v, axis=0, keepdims=True), axis=1, keepdims=True) for v in (residue, goal[...])]
    lane = lanes((1, 256))
    grads[SMALL + 2 : SMALL + 3, :] = jnp.where(lane == 0, sums[0], jnp.where(lane == 1, sums[1], 0.0))
    backward(w, g1, g2, ext1, back1, grads, r1, dkv1, dq1, 2.0 * residue, 4, 2, True)
    backward(w, g1, g2, ext0, back0, grads, r0, dkv0, dq0, back1[...], 6, 4, False)
    for by, bx, source, place in spots:
        (out_low, out_own, out_high)[by][bx, source : source + 16, :] = back0[place : place + 16, :]
    half = ROWS // 2
    kept[...] = grads[pl.ds(pl.multiple_of(core[0] * half, half), half), :]
    sent[...] = grads[pl.ds(pl.multiple_of((1 - core[0]) * half, half), half), :]


def finish_kernel(
    core, mine, other, wide, before, after,
    loss, field, embed, norm, attend, output, second, expand, reduce, decode, strip, red, turned, rows,
):
    first = core[0] == 0
    red[0 : ROWS // 2, :] = jnp.where(first, mine[...], other[...])
    red[ROWS // 2 :, :] = jnp.where(first, other[...], mine[...])
    misfit = red[SMALL + 2 : SMALL + 3, 0:1]
    energy = red[SMALL + 2 : SMALL + 3, 1:2]
    scale = 6291456.0 / energy
    loss[...] = misfit / energy
    from_tokens(scale * (wide[1] + (before[...] + after[...])), field, turned, rows)
    embed[...] = scale * reorder(strip, red[EMBED:ATTEND, :], True)
    for k in range(3):
        attend[:, 256 * k : 256 * k + 256] = scale * red[ATTEND + 256 * k : ATTEND + 256 * k + 256, :]
    output[...] = scale * red[OUTPUT:EXPAND, :]
    for k in range(2):
        expand[:, 256 * k : 256 * k + 256] = scale * red[EXPAND + 256 * k : EXPAND + 256 * k + 256, :]
    reduce[...] = scale * red[REDUCE:DECODE, :]
    decode[...] = scale * reorder(strip, red[DECODE:SMALL, :], True)
    norm[...] = scale * red[SMALL : SMALL + 1, :]
    second[...] = scale * red[SMALL + 1 : SMALL + 2, :]


def places(scalars, arrays):
    return [pl.BlockSpec(memory_space=pltpu.SMEM)] * scalars + [pl.BlockSpec(memory_space=pltpu.VMEM)] * arrays


def arr(*shape, dtype=F32):
    return jax.ShapeDtypeStruct(shape, dtype)


def call(kernel, outs, scratch, limit, **more):
    return pl.pallas_call(
        kernel,
        out_shape=outs,
        scratch_shapes=scratch,
        compiler_params=pltpu.CompilerParams(vmem_limit_bytes=limit * MIB),
        interpret=INTERPRET,
        **more,
    )


def prepare(field, target):
    scratch = [pltpu.VMEM((64, 192), F32), pltpu.VMEM((192, 128), F32)]
    return call(prepare_kernel, (arr(64, 256), arr(64, 256)), scratch, 4)(field, target)


def split_weights(weights):
    embed, _, attend, output, _, expand, reduce, decode = weights
    outs = [arr(2, *WIDTHS[name], dtype=BF16) for name in NAMES]
    inputs = (embed, attend, output, expand, reduce, decode.T)
    return call(weights_kernel, outs, [pltpu.VMEM((2, 192, 128), F32)], 14)(*inputs)


def work(core, low, own, high, goal, gains, halves):
    def V(*shape, dtype=F32):
        return pltpu.VMEM(shape, dtype)

    def kept(te, ti, n):
        return [
            V(te, 256), V(2, te, 256, dtype=BF16), V(2, te, 512, dtype=BF16), V(ti, 256), V(n * n // 2, 192, 256),
            V(ti, 256), V(ti, 256), V(ti, 512), V(ti, 256),
        ]

    scratch = [
        V(ROWS, 256),
        V(576, 256), V(576, 256), V(256, 256), V(256, 256), V(576, 512), V(256, 512), V(256, 256), V(64, 256),
        *kept(576, 256, 4), *kept(256, 64, 2),
    ]
    half = arr(ROWS // 2, 256)
    outs = (half, half, arr(3, 64, 256), arr(3, 64, 256), arr(3, 64, 256))
    args = (gains[0].reshape(1, 256), gains[1].reshape(1, 256), *halves)
    return call(main_kernel, outs, scratch, 24, in_specs=places(1, 12))(core, low, own, high, goal, *args)


def finish(core, mine, other, wide, before, after):
    outs = (
        arr(1, 1), arr(8, 8, 192), arr(192, 256), arr(1, 256), arr(256, 768), arr(256, 256), arr(1, 256),
        arr(256, 512), arr(512, 256), arr(192, 256),
    )
    scratch = [
        pltpu.VMEM((2, 192, 128), F32), pltpu.VMEM((ROWS, 256), F32),
        pltpu.VMEM((192, 128), F32), pltpu.VMEM((128, 192), F32),
    ]
    return call(finish_kernel, outs, scratch, 16, in_specs=places(1, 5))(core, mine, other, wide, before, after)


AXES = ("z", "xl", "y", "xh", "co")
GX, GY = ("z", "xl"), ("y", "xh", "co")


def shift(x, axes, step):
    count = lax.axis_size(axes)
    return lax.ppermute(x, axes, [(i, (i + step) % count) for i in range(count)])


PLANE = ("xl", "y", "xh")


def swap(x, axes):
    return lax.all_to_all(x, axes, 0, 0, tiled=True)


def shards(field, target, *weights):
    core = lax.axis_index("co").reshape(1)
    half = ROWS // 2
    swapped = [(0, 1), (1, 0)]
    halves = split_weights(weights)
    tokens, goal = prepare(field, target)
    own = jnp.stack([shift(tokens, GX, 1), tokens, shift(tokens, GX, -1)])
    low, high = shift(own, GY, 1), shift(own, GY, -1)
    kept, sent, back_low, back_own, back_high = work(core, low, own, high, goal, (weights[1], weights[4]), halves)
    total = kept + lax.ppermute(sent, "co", swapped)
    back_low, back_high = shift(back_low, GY, -1), shift(back_high, GY, 1)
    wide = back_own + (back_low + back_high)
    total = jnp.sum(swap(total.reshape(16, half // 16, 256), PLANE), axis=0)
    before, after = shift(wide[0], GX, -1), shift(wide[2], GX, 1)
    total = jnp.sum(swap(total.reshape(16, half // 256, 256), "z"), axis=0)
    total = swap(jnp.broadcast_to(total, (16,) + total.shape), "z").reshape(half // 16, 256)
    total = swap(jnp.broadcast_to(total, (16,) + total.shape), PLANE).reshape(half, 256)
    other = lax.ppermute(total, "co", swapped)
    results = finish(core, total, other, wide, before, after)
    loss, field_back, embed, norm, attend, output, second, expand, reduce, decode = results
    return loss[0, 0], field_back, embed, norm[0], attend, output, second[0], expand, reduce, decode.T


def solution(mesh):
    fine = Mesh(mesh.devices.reshape(16, 2, 4, 2, 2), AXES)
    block = P(GX, GY, None)
    in_specs = (block, block) + (P(),) * 8
    out_specs = (P(), block) + (P(),) * 8
    return jax.shard_map(shards, mesh=fine, in_specs=in_specs, out_specs=out_specs, check_vma=False)
```

```python
import jax
import jax.numpy as jnp
from jax import lax
from jax.experimental import pallas as pl
from jax.experimental.pallas import tpu as pltpu
from jax.sharding import Mesh, PartitionSpec as P

F32 = jnp.float32
BF16 = jnp.bfloat16
EPSILON = 1e-06
FACTOR = 32 ** (-0.5)
INTERPRET = False

EMBED, ATTEND, OUTPUT, EXPAND, REDUCE, DECODE, SMALL, ROWS = 0, 192, 960, 1216, 1728, 2240, 2432, 2560
MIB = 1024 * 1024


def split(x):
    high = x.astype(BF16)
    return high, (x - high.astype(F32)).astype(BF16)


def dot(a, b, ca=1, cb=0):
    dims = (((ca,), (cb,)), ((), ()))

    def one(left, right):
        return lax.dot_general(left, right, dims, preferred_element_type=F32)

    return one(a[0], b[0]) + (one(a[0], b[1]) + one(a[1], b[0]))


def lanes(shape):
    return lax.broadcasted_iota(jnp.int32, shape, 1)


def over_components(x):
    x = x + pltpu.roll(x, 128, 1)
    return x + pltpu.roll(x, 64, 1)


def to_tokens(block_ref, out_ref, rows_ref, turned_ref):
    for px in range(2):
        for py in range(2):
            for dx in range(4):
                row = (px * 2 + py) * 16 + dx * 4
                rows_ref[row : row + 4, :] = block_ref[px * 4 + dx, py * 4 : py * 4 + 4, :]
    turned_ref[:, 0:64] = rows_ref[...].T
    turned_ref[:, 64:128] = jnp.zeros((192, 64), F32)
    lane = lanes((16, 128))
    halves = [[jnp.zeros((16, 128), F32) for _ in range(2)] for _ in range(4)]
    for c in range(3):
        for dz in range(4):
            piece = turned_ref[pl.ds(c * 64 + dz, 16, stride=4), :]
            place = c * 64 + dz * 16
            half, low = place // 128, place % 128
            chosen = (lane >= low) & (lane < low + 16)
            for column in range(4):
                shift = (low - column * 16) % 128
                moved = pltpu.roll(piece, shift, 1) if shift else piece
                halves[column][half] = jnp.where(chosen, moved, halves[column][half])
    for column in range(4):
        for half in range(2):
            out_ref[column * 16 : column * 16 + 16, half * 128 : half * 128 + 128] = halves[column][half]


def from_tokens(total, out_ref, turned_ref, rows_ref):
    lane = lanes((16, 128))
    for c in range(3):
        for dz in range(4):
            place = c * 64 + dz * 16
            half, low = place // 128, place % 128
            piece = jnp.zeros((16, 128), F32)
            for column in range(4):
                source = total[column * 16 : column * 16 + 16, half * 128 : half * 128 + 128]
                shift = (column * 16 - low) % 128
                moved = pltpu.roll(source, shift, 1) if shift else source
                chosen = (lane >= column * 16) & (lane < column * 16 + 16)
                piece = jnp.where(chosen, moved, piece)
            turned_ref[pl.ds(c * 64 + dz, 16, stride=4), :] = piece
    rows_ref[...] = turned_ref[...].T
    for px in range(2):
        for py in range(2):
            for dx in range(4):
                row = (px * 2 + py) * 16 + dx * 4
                out_ref[px * 4 + dx, py * 4 : py * 4 + 4, :] = rows_ref[row : row + 4, :]


def inner_rows(ref, m, n, dx=0, dy=0):
    parts = [ref[((X + 1 + dx) * m + 1 + dy) * 16 : ((X + 1 + dx) * m + 1 + dy + n) * 16, :] for X in range(n)]
    return jnp.concatenate(parts, axis=0)


def add_inner(ref, m, n, value, dx=0, dy=0):
    for X in range(n):
        start = ((X + 1 + dx) * m + 1 + dy) * 16
        ref[start : start + n * 16, :] += value[X * n * 16 : (X + 1) * n * 16]


def neighbours(ext_ref, m, n):
    count = n * n * 16
    lane = lanes((count, 256))
    row = lax.broadcasted_iota(jnp.int32, (count, 256), 0)
    dx, dy, dz, pz = (lane // 4) % 4, lane % 4, (lane // 16) % 4, row % 16
    here = inner_rows(ext_ref, m, n)
    roll = pltpu.roll
    east = jnp.where(dx < 3, roll(here, 252, 1), roll(inner_rows(ext_ref, m, n, 1, 0), 12, 1))
    west = jnp.where(dx > 0, roll(here, 4, 1), roll(inner_rows(ext_ref, m, n, -1, 0), 244, 1))
    north = jnp.where(dy < 3, roll(here, 255, 1), roll(inner_rows(ext_ref, m, n, 0, 1), 3, 1))
    south = jnp.where(dy > 0, roll(here, 1, 1), roll(inner_rows(ext_ref, m, n, 0, -1), 253, 1))
    above = jnp.where(pz == 15, 0.0, roll(here, count - 1, 0))
    below = jnp.where(pz == 0, 0.0, roll(here, 1, 0))
    upper = jnp.where(dz < 3, roll(here, 240, 1), roll(above, 48, 1))
    lower = jnp.where(dz > 0, roll(here, 16, 1), roll(below, 208, 1))
    speeds = [over_components(jnp.where(lane // 64 == k, here, 0.0)) for k in range(3)]
    return here, (east, west, north, south, upper, lower), speeds


def stencil(ext_ref, m, n):
    here, (east, west, north, south, upper, lower), speeds = neighbours(ext_ref, m, n)
    laplace = (east + west) + (north + south) + (upper + lower) - 6.0 * here
    carried = speeds[0] * (east - west) + speeds[1] * (north - south) + speeds[2] * (upper - lower)
    return here + 0.05 * (laplace - carried)


def stencil_back(ext_ref, back_ref, g, m, n):
    count = n * n * 16
    lane = lanes((count, 256))
    row = lax.broadcasted_iota(jnp.int32, (count, 256), 0)
    dx, dy, dz, pz = (lane // 4) % 4, lane % 4, (lane // 16) % 4, row % 16
    comp = lane // 64
    roll = pltpu.roll
    here, (east, west, north, south, upper, lower), speeds = neighbours(ext_ref, m, n)
    scaled = 0.05 * g
    own = 0.7 * g
    for k, (ahead, behind) in enumerate(((east, west), (north, south), (upper, lower))):
        own = own - jnp.where(comp == k, over_components(scaled * (ahead - behind)), 0.0)
    plus, minus = scaled * (1.0 - speeds[0]), scaled * (1.0 + speeds[0])
    own = own + jnp.where(dx > 0, roll(plus, 4, 1), 0.0) + jnp.where(dx < 3, roll(minus, 252, 1), 0.0)
    add_inner(back_ref, m, n, jnp.where(dx == 0, roll(plus, 244, 1), 0.0), 1, 0)
    add_inner(back_ref, m, n, jnp.where(dx == 3, roll(minus, 12, 1), 0.0), -1, 0)
    plus, minus = scaled * (1.0 - speeds[1]), scaled * (1.0 + speeds[1])
    own = own + jnp.where(dy > 0, roll(plus, 1, 1), 0.0) + jnp.where(dy < 3, roll(minus, 255, 1), 0.0)
    add_inner(back_ref, m, n, jnp.where(dy == 0, roll(plus, 253, 1), 0.0), 0, 1)
    add_inner(back_ref, m, n, jnp.where(dy == 3, roll(minus, 3, 1), 0.0), 0, -1)
    plus, minus = scaled * (1.0 - speeds[2]), scaled * (1.0 + speeds[2])
    own = own + jnp.where(dz > 0, roll(plus, 16, 1), 0.0) + jnp.where(dz < 3, roll(minus, 240, 1), 0.0)
    across = jnp.where(dz == 0, roll(plus, 208, 1), 0.0)
    own = own + jnp.where(pz == 0, 0.0, roll(across, 1, 0))
    across = jnp.where(dz == 3, roll(minus, 48, 1), 0.0)
    own = own + jnp.where(pz == 15, 0.0, roll(across, count - 1, 0))
    add_inner(back_ref, m, n, own)


def rms(x):
    return lax.rsqrt(jnp.mean(x * x, axis=1, keepdims=True) + EPSILON)


def rms_back(values, scale, gain, cotangent):
    weighted = cotangent * gain
    shared = jnp.mean(weighted * values, axis=1, keepdims=True)
    return scale * (weighted - values * (scale * scale * shared))


def pair(ref, start, size):
    return ref[0, pl.ds(start, size), :], ref[1, pl.ds(start, size), :]


def put(ref, start, value):
    high, low = split(value)
    ref[0, pl.ds(start, value.shape[0]), :] = high
    ref[1, pl.ds(start, value.shape[0]), :] = low


def both(ref):
    return ref[0], ref[1]


def head_mask():
    row = lax.broadcasted_iota(jnp.int32, (128, 256), 0)
    return row // 16 == lanes((128, 256)) // 32


def pair_mask():
    key = lax.broadcasted_iota(jnp.int32, (192, 256), 0) // 16 % 4
    query = lanes((192, 256)) // 128
    return (key >= query) & (key < query + 3)


def by_head(x, mask):
    wide = [jnp.where(mask, jnp.concatenate([x[k * 16 : k * 16 + 16]] * 8, axis=0), 0.0) for k in range(2)]
    return split(jnp.concatenate(wide, axis=0))


def from_heads(x, mask):
    columns = []
    for k in range(2):
        kept = jnp.where(mask, x[128 * k : 128 * k + 128], 0.0)
        total = [kept[head * 16 : head * 16 + 16] for head in range(8)]
        while len(total) > 1:
            total = [total[i] + total[i + 1] for i in range(0, len(total), 2)]
        columns.append(total[0])
    return jnp.concatenate(columns, axis=0)


def key_rows(X, Y, m):
    return [((X + dx) * m + Y) * 16 for dx in range(3)]


def gather(ref, starts, low, high):
    def one(which):
        return jnp.concatenate([ref[which, s : s + 64, low:high] for s in starts], axis=0)

    return one(0), one(1)


def pairs_of(n):
    return [(X, Y) for X in range(n) for Y in range(0, n, 2)]


def forward(w, g1, g2, ext_ref, r, m, n, chunk):
    (tok, nrm, kv, q, wts, att, mid, h, late) = r

    def embed(i, _):
        start = pl.multiple_of(i * chunk, chunk)
        tokens = dot(split(ext_ref[pl.ds(start, chunk), :]), both(w["embed"]))
        tok[pl.ds(start, chunk), :] = tokens
        normed = tokens * rms(tokens) * g1
        put(nrm, start, normed)
        put(kv, start, dot(pair(nrm, start, chunk), (w["attend"][0, :, 256:], w["attend"][1, :, 256:])))
        return 0

    lax.fori_loop(0, m * m * 16 // chunk, embed, 0)
    normed_in = inner_rows(nrm.at[0], m, n), inner_rows(nrm.at[1], m, n)
    q[...] = dot(normed_in, (w["attend"][0, :, :256], w["attend"][1, :, :256]))
    mask = head_mask()

    allowed = pair_mask()

    def attend(pairs):
        results = []
        for X, Y in pairs:
            starts = key_rows(X, Y, m)
            wide = by_head(q[(X * n + Y) * 16 : (X * n + Y) * 16 + 32, :], mask)
            weights = jnp.where(allowed, jnp.exp(dot(gather(kv, starts, 0, 256), wide, 1, 1) * FACTOR), 0.0)
            weights = weights / jnp.sum(weights, axis=0, keepdims=True)
            results.append((weights, from_heads(dot(split(weights), gather(kv, starts, 256, 512), 0, 0), mask)))
        for (X, Y), (weights, attended) in zip(pairs, results):
            wts[X * (n // 2) + Y // 2] = weights
            att[(X * n + Y) * 16 : (X * n + Y) * 16 + 32, :] = attended

    attend(pairs_of(n))
    middle = inner_rows(tok, m, n) + dot(split(att[...]), both(w["output"]))
    mid[...] = middle
    hidden = dot(split(middle * rms(middle) * g2), both(w["expand"]))
    h[...] = hidden
    active = hidden / (1.0 + jnp.exp(-hidden))
    final = middle + dot(split(active), both(w["reduce"]))
    late[...] = final
    return dot(split(final), both(w["decode"]), 1, 1)


def add_rows(ref, start, value, first):
    size = value.shape[0]
    if first:
        ref[start : start + size, :] = value
    else:
        ref[start : start + size, :] += value


def reorder(strip, source, inverse=False):
    places = [(c * 64 + dz * 16, c * 64 + dz) for c in range(3) for dz in range(4)]
    halves = []
    for k in range(2):
        part = source[:, 128 * k : 128 * k + 128]
        if inverse:
            for place, row in places:
                strip[k, pl.ds(row, 16, stride=4), :] = part[place : place + 16]
            halves.append(strip[k])
        else:
            strip[k] = part
            halves.append(jnp.concatenate([strip[k, pl.ds(row, 16, stride=4), :] for _, row in places], axis=0))
    return jnp.concatenate(halves, axis=1)


def backward(w, g1, g2, ext_ref, back_ref, grads, r, dkv, dq, g, m, n, first):
    (tok, nrm, kv, q, wts, att, mid, h, late) = r
    dclosure = split(0.1 * g)
    add_rows(grads, DECODE, dot(dclosure, split(late[...]), 0, 0)[:192], first)
    dmid = dot(dclosure, both(w["decode"]))
    back = split(dmid)
    hidden = h[...]
    gate = 1.0 / (1.0 + jnp.exp(-hidden))
    add_rows(grads, REDUCE, dot(split(hidden * gate), back, 0, 0), first)
    dhidden = split(dot(back, both(w["reduce"]), 1, 1) * (gate * (1.0 + hidden * (1.0 - gate))))
    middle = mid[...]
    scale = rms(middle)
    second = split(middle * scale * g2)
    add_rows(grads, EXPAND, dot(second, (dhidden[0][:, :256], dhidden[1][:, :256]), 0, 0), first)
    add_rows(grads, EXPAND + 256, dot(second, (dhidden[0][:, 256:], dhidden[1][:, 256:]), 0, 0), first)
    dsecond = dot(dhidden, both(w["expand"]), 1, 1)
    add_rows(grads, SMALL + 1, jnp.sum(dsecond * middle * scale, axis=0, keepdims=True), first)
    dmid = dmid + rms_back(middle, scale, g2, dsecond)
    back = split(dmid)
    add_rows(grads, OUTPUT, dot(split(att[...]), back, 0, 0), first)
    att[...] = dot(back, both(w["output"]), 1, 1)
    dkv[...] = jnp.zeros(dkv.shape, F32)
    mask = head_mask()

    def attend(pairs):
        results = []
        for X, Y in pairs:
            starts = key_rows(X, Y, m)
            here = slice((X * n + Y) * 16, (X * n + Y) * 16 + 32)
            wide, dwide = by_head(q[here, :], mask), by_head(att[here, :], mask)
            weights = wts[X * (n // 2) + Y // 2]
            dweights = dot(gather(kv, starts, 256, 512), dwide, 1, 1)
            common = jnp.sum(weights * dweights, axis=0, keepdims=True)
            dscores = split(weights * (dweights - common) * FACTOR)
            dqueries = from_heads(dot(dscores, gather(kv, starts, 0, 256), 0, 0), mask)
            results.append((dqueries, dot(dscores, wide), dot(split(weights), dwide)))
        for (X, Y), (dqueries, dkeys, dvals) in zip(pairs, results):
            dq[(X * n + Y) * 16 : (X * n + Y) * 16 + 32, :] = dqueries
            for k, s in enumerate(key_rows(X, Y, m)):
                dkv[s : s + 64, 0:256] += dkeys[k * 64 : k * 64 + 64]
                dkv[s : s + 64, 256:512] += dvals[k * 64 : k * 64 + 64]

    attend(pairs_of(n))
    normed_in = inner_rows(nrm.at[0], m, n), inner_rows(nrm.at[1], m, n)
    dquery = split(dq[...])
    add_rows(grads, ATTEND, dot(normed_in, dquery, 0, 0), first)
    back_ref[...] = jnp.zeros(back_ref.shape, F32)
    add_inner(back_ref, m, n, dot(dquery, (w["attend"][0, :, :256], w["attend"][1, :, :256]), 1, 1))
    total = dkv[...]
    halves = [split(total[:, 0:256]), split(total[:, 256:512])]
    normed = both(nrm)
    for k in range(2):
        add_rows(grads, ATTEND + 256 + 256 * k, dot(normed, halves[k], 0, 0), first)
    dnormed = back_ref[...]
    for k in range(2):
        low, high = 256 + 256 * k, 512 + 256 * k
        dnormed = dnormed + dot(halves[k], (w["attend"][0, :, low:high], w["attend"][1, :, low:high]), 1, 1)
    tokens = tok[...]
    scale = rms(tokens)
    add_rows(grads, SMALL, jnp.sum(dnormed * tokens * scale, axis=0, keepdims=True), first)
    back_ref[...] = rms_back(tokens, scale, g1, dnormed)
    add_inner(back_ref, m, n, dmid)
    dtokens = split(back_ref[...])
    add_rows(grads, EMBED, dot(split(ext_ref[...]), dtokens, 0, 0)[:192], first)
    return dtokens


def backward_field(embed, ext_ref, back_ref, dtokens, g, m, n):
    back_ref[...] = dot(dtokens, both(embed), 1, 1)
    stencil_back(ext_ref, back_ref, g, m, n)


NAMES = ("embed", "attend", "output", "expand", "reduce", "decode")
WIDTHS = {"embed": (256, 256), "attend": (256, 768), "output": (256, 256), "expand": (256, 512), "reduce": (512, 256), "decode": (256, 256)}


def weights_kernel(*refs):
    inputs, w, strip = dict(zip(NAMES, refs[:6])), dict(zip(NAMES, refs[6:12])), refs[12]
    for name in NAMES:
        if name in ("embed", "decode"):
            put(w[name], 0, reorder(strip, inputs[name][...]))
            put(w[name], 192, jnp.zeros((64, 256), F32))
        else:
            put(w[name], 0, inputs[name][...])


SPOTS = [
    (by, bx, (px * 2 + py) * 16, ((2 * bx + px) * 6 + 2 * by + py) * 16)
    for by in range(3) for bx in range(3) for px in range(2) for py in range(2)
]


def field_kernel(embed, ext0, g0, dtokens, out_low, out_own, out_high, back_ref):
    backward_field(embed, ext0, back_ref, both(dtokens), g0[...], 6, 4)
    for by, bx, source, place in SPOTS:
        (out_low, out_own, out_high)[by][bx, source : source + 16, :] = back_ref[place : place + 16, :]


def main_kernel(*refs):
    (core, low, own, high, goal, gain1, gain2) = refs[:7]
    w = dict(zip(NAMES, refs[7:13]))
    (kept, sent, ext0, g0, dtokens0) = refs[13:18]
    scratch = list(refs[18:])
    grads = scratch.pop(0)
    back0, ext1, back1, dkv0, dkv1, dq0, dq1 = scratch[:7]
    r0, r1 = scratch[7:16], scratch[16:25]
    g1, g2 = gain1[...], gain2[...]
    for by, bx, source, place in SPOTS:
        ext0[place : place + 16, :] = (low, own, high)[by][bx, source : source + 16, :]
    ext1[...] = stencil(ext0, 6, 4) + 0.1 * forward(w, g1, g2, ext0, r0, 6, 4, 576)
    final = stencil(ext1, 4, 2) + 0.1 * forward(w, g1, g2, ext1, r1, 4, 2, 256)
    residue = final - goal[...]
    grads[SMALL:ROWS, :] = jnp.zeros((ROWS - SMALL, 256), F32)
    sums = [jnp.sum(jnp.sum(v * v, axis=0, keepdims=True), axis=1, keepdims=True) for v in (residue, goal[...])]
    lane = lanes((1, 256))
    grads[SMALL + 2 : SMALL + 3, :] = jnp.where(lane == 0, sums[0], jnp.where(lane == 1, sums[1], 0.0))
    g = 2.0 * residue
    dtokens = backward(w, g1, g2, ext1, back1, grads, r1, dkv1, dq1, g, 4, 2, True)
    backward_field(w["embed"], ext1, g0, dtokens, g, 4, 2)
    dtokens0[0], dtokens0[1] = backward(w, g1, g2, ext0, back0, grads, r0, dkv0, dq0, g0[...], 6, 4, False)
    half = ROWS // 2
    kept[...] = grads[pl.ds(pl.multiple_of(core[0] * half, half), half), :]
    sent[...] = grads[pl.ds(pl.multiple_of((1 - core[0]) * half, half), half), :]


def finish_kernel(
    core, mine, other, wide, before, after,
    loss, field, embed, norm, attend, output, second, expand, reduce, decode, strip, red, turned, rows,
):
    first = core[0] == 0
    red[0 : ROWS // 2, :] = jnp.where(first, mine[...], other[...])
    red[ROWS // 2 :, :] = jnp.where(first, other[...], mine[...])
    misfit = red[SMALL + 2 : SMALL + 3, 0:1]
    energy = red[SMALL + 2 : SMALL + 3, 1:2]
    scale = 6291456.0 / energy
    loss[...] = misfit / energy
    from_tokens(scale * (wide[1] + (before[...] + after[...])), field, turned, rows)
    embed[...] = scale * reorder(strip, red[EMBED:ATTEND, :], True)
    for k in range(3):
        attend[:, 256 * k : 256 * k + 256] = scale * red[ATTEND + 256 * k : ATTEND + 256 * k + 256, :]
    output[...] = scale * red[OUTPUT:EXPAND, :]
    for k in range(2):
        expand[:, 256 * k : 256 * k + 256] = scale * red[EXPAND + 256 * k : EXPAND + 256 * k + 256, :]
    reduce[...] = scale * red[REDUCE:DECODE, :]
    decode[...] = scale * reorder(strip, red[DECODE:SMALL, :], True)
    norm[...] = scale * red[SMALL : SMALL + 1, :]
    second[...] = scale * red[SMALL + 1 : SMALL + 2, :]


def places(scalars, arrays):
    return [pl.BlockSpec(memory_space=pltpu.SMEM)] * scalars + [pl.BlockSpec(memory_space=pltpu.VMEM)] * arrays


def arr(*shape, dtype=F32):
    return jax.ShapeDtypeStruct(shape, dtype)


def call(kernel, outs, scratch, limit, **more):
    return pl.pallas_call(
        kernel,
        out_shape=outs,
        scratch_shapes=scratch,
        compiler_params=pltpu.CompilerParams(vmem_limit_bytes=limit * MIB),
        interpret=INTERPRET,
        **more,
    )


def prepare(block):
    scratch = [pltpu.VMEM((64, 192), F32), pltpu.VMEM((192, 128), F32)]
    return call(to_tokens, arr(64, 256), scratch, 4)(block)


def split_weights(weights):
    embed, _, attend, output, _, expand, reduce, decode = weights
    outs = [arr(2, *WIDTHS[name], dtype=BF16) for name in NAMES]
    inputs = (embed, attend, output, expand, reduce, decode.T)
    return call(weights_kernel, outs, [pltpu.VMEM((2, 192, 128), F32)], 14)(*inputs)


def work(core, low, own, high, goal, gains, halves):
    def V(*shape, dtype=F32):
        return pltpu.VMEM(shape, dtype)

    def kept(te, ti, n):
        return [
            V(te, 256), V(2, te, 256, dtype=BF16), V(2, te, 512, dtype=BF16), V(ti, 256), V(n * n // 2, 192, 256),
            V(ti, 256), V(ti, 256), V(ti, 512), V(ti, 256),
        ]

    scratch = [
        V(ROWS, 256),
        V(576, 256), V(256, 256), V(256, 256), V(576, 512), V(256, 512), V(256, 256), V(64, 256),
        *kept(576, 256, 4), *kept(256, 64, 2),
    ]
    half = arr(ROWS // 2, 256)
    outs = (half, half, arr(576, 256), arr(256, 256), arr(2, 576, 256, dtype=BF16))
    args = (gains[0].reshape(1, 256), gains[1].reshape(1, 256), *halves)
    return call(main_kernel, outs, scratch, 24, in_specs=places(1, 12))(core, low, own, high, goal, *args)


def adjoint(embed, ext0, g0, dtokens):
    outs = [arr(3, 64, 256)] * 3
    return call(field_kernel, outs, [pltpu.VMEM((576, 256), F32)], 10)(embed, ext0, g0, dtokens)


def finish(core, mine, other, wide, before, after):
    outs = (
        arr(1, 1), arr(8, 8, 192), arr(192, 256), arr(1, 256), arr(256, 768), arr(256, 256), arr(1, 256),
        arr(256, 512), arr(512, 256), arr(192, 256),
    )
    scratch = [
        pltpu.VMEM((2, 192, 128), F32), pltpu.VMEM((ROWS, 256), F32),
        pltpu.VMEM((192, 128), F32), pltpu.VMEM((128, 192), F32),
    ]
    return call(finish_kernel, outs, scratch, 16, in_specs=places(1, 5))(core, mine, other, wide, before, after)


AXES = ("z", "xl", "y", "xh", "co")
GX, GY = ("z", "xl"), ("y", "xh", "co")


def shift(x, axes, step):
    count = lax.axis_size(axes)
    return lax.ppermute(x, axes, [(i, (i + step) % count) for i in range(count)])


PLANE = ("xl", "y", "xh")


def swap(x, axes):
    return lax.all_to_all(x, axes, 0, 0, tiled=True)


def shards(field, target, *weights):
    core = lax.axis_index("co").reshape(1)
    half = ROWS // 2
    swapped = [(0, 1), (1, 0)]
    halves = split_weights(weights)
    tokens = prepare(field)
    goal = prepare(target)
    own = jnp.stack([shift(tokens, GX, 1), tokens, shift(tokens, GX, -1)])
    low, high = shift(own, GY, 1), shift(own, GY, -1)
    kept, sent, ext0, g0, dtokens = work(core, low, own, high, goal, (weights[1], weights[4]), halves)
    total = kept + lax.ppermute(sent, "co", swapped)
    back_low, back_own, back_high = adjoint(halves[0], ext0, g0, dtokens)
    back_low, back_high = shift(back_low, GY, -1), shift(back_high, GY, 1)
    wide = back_own + (back_low + back_high)
    total = jnp.sum(swap(total.reshape(16, half // 16, 256), PLANE), axis=0)
    before, after = shift(wide[0], GX, -1), shift(wide[2], GX, 1)
    total = jnp.sum(swap(total.reshape(16, half // 256, 256), "z"), axis=0)
    total = swap(jnp.broadcast_to(total, (16,) + total.shape), "z").reshape(half // 16, 256)
    total = swap(jnp.broadcast_to(total, (16,) + total.shape), PLANE).reshape(half, 256)
    other = lax.ppermute(total, "co", swapped)
    results = finish(core, total, other, wide, before, after)
    loss, field_back, embed, norm, attend, output, second, expand, reduce, decode = results
    return loss[0, 0], field_back, embed, norm[0], attend, output, second[0], expand, reduce, decode.T


def solution(mesh):
    fine = Mesh(mesh.devices.reshape(16, 2, 4, 2, 2), AXES)
    block = P(GX, GY, None)
    in_specs = (block, block) + (P(),) * 8
    out_specs = (P(), block) + (P(),) * 8
    return jax.shard_map(shards, mesh=fine, in_specs=in_specs, out_specs=out_specs, check_vma=False)
```
